256 devices in a mesh: blk: 16 (over z, y_lo), grp: 16 (over x, y_hi, core).
Axes of the slice: x: 4, y: 4 (y_hi: 2, y_lo: 2; y = y_hi * 2 + y_lo), z: 8, core: 2. Of those that a mesh axis runs over, the one named last changes fastest.
Arguments:
- frames: bfloat16 [16, 4096, 1024], P('grp', 'blk'), may hold values from -16 to 16
- utt_lengths: int32 [8], replicated, may hold values from 1 to 16384, 65536 in all
- attn_gain: float32 [1024], replicated, may hold values from 0.25 to 1.75
- w_qkv: bfloat16 [1024, 3072], P(None, 'grp'), may hold values from -4 to 4
- w_out: bfloat16 [1024, 1024], replicated, may hold values from -0.375 to 0.375
- conv_gain: float32 [1024], replicated, may hold values from 0.25 to 1.75
- w_glu: bfloat16 [1024, 2048], replicated, may hold values from -0.1875 to 0.1875
- w_depth: float32 [31, 1024], replicated, may hold values from -1 to 1
- depth_gain: float32 [1024], replicated, may hold values from 0.25 to 1.75
- w_proj: bfloat16 [1024, 1024], replicated, may hold values from -0.1875 to 0.1875
Outputs:
- block_out: bfloat16 [16, 4096, 1024], P('grp', 'blk')
The draws below stay inside these ranges and needn't reach their ends.
Inputs may be any that keep to these rules, and one draw needn't show every extreme that they name: `utt_lengths`: they sum to 65536 and the longest is exactly 16384.
All inputs are finite; a program needn't handle non-finite values.
Results may differ from the reference program's by a relative error of at most 0.0095.
Values may be sent and summed in bfloat16 or wider, within the bound.
A program may use at most 192 MiB of HBM per device.

```python
import math
import jax
import jax.numpy as jnp
import numpy as np
from jax import lax

D = 1024
HEADS = 16
KERNEL = 31
WINDOW = 4096
GROUPS = 16
TOKENS = 65536
UTT_MOST = 16384
UTTERANCES = 8


def draw_frames(key, part):
    base_key = jax.random.fold_in(jax.random.fold_in(key, 11), 0)
    drawn = jax.random.normal(base_key, (GROUPS, WINDOW, D), jnp.float32)
    return jnp.clip(drawn, -16.0, 16.0).astype(jnp.bfloat16)


def draw_w_qkv(key, part):
    drawn = jax.random.normal(jax.random.fold_in(key, 23), (D, HEADS, 3, D // HEADS), jnp.float32) * (1.4 / math.sqrt(D))
    return jnp.clip(drawn.reshape(D, 3 * D), -4.0, 4.0).astype(jnp.bfloat16)


def length_profile(amount, total, most, slope):
    loads = [(1 << 20) // math.isqrt(grade ** slope) + 1 for grade in range(2, amount + 1)]
    surplus, counts = total - most - (amount - 1), [1] * (amount - 1)
    while surplus > 0:
        candidates = [i for i in range(amount - 1) if counts[i] < most]
        pool, remaining = sum([loads[i] for i in candidates]), surplus
        for i in candidates:
            addition = min(most - counts[i], max(1, remaining * loads[i] // pool), surplus)
            counts[i] = counts[i] + addition
            surplus = surplus - addition
    return np.array([most] + counts)


def ragged(own_key, count, total, reach, slope):
    if count == 2:
        one = jax.random.randint(own_key, (), max(1, total - reach), min(reach, total - 1) + 1)
        return jnp.stack([one, total - one])
    sizes = jnp.asarray(length_profile(count, total, reach, slope), jnp.int32)
    pairs = (count - 1) // 2
    donor, taker = sizes[1:1 + 2 * pairs:2], sizes[2:2 + 2 * pairs:2]
    slack = jnp.minimum(donor - 1, reach - taker)
    moved = jax.random.randint(jax.random.fold_in(own_key, 1), (pairs,), 0, 1 << 20) % (slack + 1)
    sizes = sizes.at[1:1 + 2 * pairs:2].set(donor - moved).at[2:2 + 2 * pairs:2].set(taker + moved)
    return sizes[jax.random.permutation(jax.random.fold_in(own_key, 2), count)]


def centred(stream_key, shape, scale, limit, held_as=jnp.bfloat16):
    values = scale * jax.random.normal(stream_key, shape, jnp.float32)
    return jnp.clip(values, min=-limit, max=limit).astype(held_as)


def setup_inputs(seed: int = 0) -> dict:
    splits = jax.random.split(jax.random.key(seed), 11)
    return {
        "frames": draw_frames(jax.random.fold_in(splits[10], 71), 0),
        "utt_lengths": ragged(splits[1], UTTERANCES, TOKENS, UTT_MOST, 2).astype(jnp.int32),
        "attn_gain": jnp.clip(1.0 + 0.15 * jax.random.normal(splits[2], (D,), jnp.float32), 0.25, 1.75),
        "w_qkv": draw_w_qkv(jax.random.fold_in(splits[10], 71), 0),
        "w_out": centred(splits[4], (D, D), (D // 4) ** -0.5, 0.375),
        "conv_gain": jnp.clip(1.0 + 0.15 * jax.random.normal(splits[5], (D,), jnp.float32), 0.25, 1.75),
        "w_glu": centred(splits[6], (D, 2 * D), D ** -0.5, 0.1875),
        "w_depth": centred(splits[7], (KERNEL, D), KERNEL ** -0.5, 1.0, jnp.float32),
        "depth_gain": jnp.clip(1.0 + 0.15 * jax.random.normal(splits[8], (D,), jnp.float32), 0.25, 1.75),
        "w_proj": centred(splits[9], (D, D), D ** -0.5, 0.1875),
    }


epsilon = 1e-05
big_negative = -1e+30

def normalize(values, row_gain):
    center = values - lax.optimization_barrier(jnp.mean(values, axis=-1, keepdims=True))
    spread = lax.optimization_barrier(jnp.mean(center * center, axis=-1, keepdims=True))
    return center * lax.rsqrt(spread + epsilon) * row_gain

def segment_of(utt_lengths, positions):
    starts = jnp.cumsum(utt_lengths) - utt_lengths
    started = (starts[None, :] <= positions[:, None]).astype(jnp.int32)
    return lax.optimization_barrier(jnp.sum(started, axis=1)) - 1

def one_head(head_qkv, seg_row, score_scale):
    scores = jnp.dot(head_qkv[0], head_qkv[1].T, preferred_element_type=jnp.float32) * score_scale
    allowed = seg_row[:, None] == seg_row[None, :]
    row_max = lax.optimization_barrier(jnp.max(jnp.where(allowed, scores, big_negative), axis=1, keepdims=True))
    weights = jnp.where(allowed, jnp.exp(scores - row_max), 0.0)
    row_total = lax.optimization_barrier(jnp.sum(weights, axis=1, keepdims=True))
    mixed_values = jnp.dot(weights.astype(jnp.bfloat16), head_qkv[2], preferred_element_type=jnp.float32)
    return mixed_values / row_total

def reference(frames, utt_lengths, attn_gain, w_qkv, w_out, conv_gain, w_glu, w_depth, depth_gain, w_proj):
    head_width = D // HEADS
    kernel_half = (KERNEL - 1) // 2
    score_scale = head_width ** (-0.5)
    flat_frames = frames.reshape(TOKENS, D)
    flat_float = flat_frames.astype(jnp.float32)
    frame_seg = segment_of(utt_lengths, jnp.arange(TOKENS, dtype=jnp.int32))
    normed = normalize(flat_float, attn_gain).astype(jnp.bfloat16)
    qkv_rows = jnp.dot(normed, w_qkv, preferred_element_type=jnp.float32).astype(jnp.bfloat16)
    arranged = jnp.transpose(qkv_rows.reshape(GROUPS, WINDOW, HEADS, 3, head_width), (0, 2, 3, 1, 4))
    group_seg = frame_seg.reshape(GROUPS, WINDOW)

    def one_group(operands):
        group_qkv, seg_row = operands
        return lax.map(lambda head_qkv: one_head(head_qkv, seg_row, score_scale), group_qkv)
    heads_out = lax.map(one_group, (arranged, group_seg))
    attended = jnp.transpose(heads_out, (0, 2, 1, 3)).reshape(TOKENS, D).astype(jnp.bfloat16)
    residual = (flat_float + jnp.dot(attended, w_out, preferred_element_type=jnp.float32)).astype(jnp.bfloat16)
    residual = lax.optimization_barrier(residual)
    conv_in = normalize(residual.astype(jnp.float32), conv_gain).astype(jnp.bfloat16)
    projected = jnp.dot(conv_in, w_glu, preferred_element_type=jnp.float32)
    gated = (projected[:, :D] * jax.nn.sigmoid(projected[:, D:])).astype(jnp.bfloat16)
    gated = lax.optimization_barrier(gated)
    padded = jnp.pad(gated.astype(jnp.float32), ((kernel_half, kernel_half), (0, 0)))
    pad_seg = segment_of(utt_lengths, jnp.arange(-kernel_half, TOKENS + kernel_half, dtype=jnp.int32))
    mixed_conv = jnp.zeros((TOKENS, D), jnp.float32)
    for offset in range(KERNEL):
        same_seg = (pad_seg[offset:offset + TOKENS] == frame_seg)[:, None]
        mixed_conv = mixed_conv + jnp.where(same_seg, padded[offset:offset + TOKENS] * w_depth[offset], 0.0)
    normed_conv = normalize(mixed_conv, depth_gain)
    activated = (normed_conv * jax.nn.sigmoid(normed_conv)).astype(jnp.bfloat16)
    result = (residual.astype(jnp.float32) + jnp.dot(activated, w_proj, preferred_element_type=jnp.float32)).astype(jnp.bfloat16)
    return result.reshape(GROUPS, WINDOW, D)
```

```python
import functools
import math

import jax
import jax.numpy as jnp
from jax import lax
from jax.experimental import pallas as pl
from jax.experimental.pallas import tpu as pltpu
from jax.sharding import PartitionSpec as P

HEADS = 16
MESH = pl.DeviceIdType.MESH

epsilon = 1e-05
big_negative = -1e30


def normalize(values, row_gain):
    center = values - jnp.mean(values, axis=-1, keepdims=True)
    spread = jnp.mean(center * center, axis=-1, keepdims=True)
    return center * lax.rsqrt(spread + epsilon) * row_gain


def segment_of(utt_lengths, positions):
    starts = jnp.cumsum(utt_lengths) - utt_lengths
    started = (starts[None, :] <= positions[:, None]).astype(jnp.int32)
    return jnp.sum(started, axis=1) - 1


def attention_kernel(
    utt_ref, frames_ref, gain_ref, w_ref,
    att_ref,
    from_low, from_high, w_pair, stage, qkv, query, keys, scores, out_stage,
    load_sem, low_send, low_recv, high_send, high_recv, w_send, w_recv, core_send, core_recv,
    swap_send, swap_recv, out_send, out_recv,
):
    half = from_low.shape[1]
    rows = 2 * half
    blk = lax.axis_index("blk")
    grp = lax.axis_index("grp")
    z, y_low = blk // 2, blk % 2
    x, y_high, core = grp // 4, (grp // 2) % 2, grp % 2
    dx, dy = z % 4, z // 4
    w_target = ((x + 4 - dx) % 4) * 4 + ((y_high + dy) % 2) * 2 + core
    w_source = ((x + dx) % 4) * 4 + ((y_high + dy) % 2) * 2 + core
    my_head = ((x + dx) % 4) * 4 + ((y_high + dy) % 2) * 2 + y_low
    other_core = grp + 1 - 2 * core
    partner = blk + 1 - 2 * y_low
    z_up = (blk + 2) % 16
    z_down = (blk + 14) % 16

    def place(b, g):
        return {"blk": b, "grp": g}

    loads = [
        pltpu.make_async_copy(frames_ref.at[pl.ds(0, half)], from_low.at[7], load_sem.at[0]),
        pltpu.make_async_copy(frames_ref.at[pl.ds(half, half)], from_high.at[7], load_sem.at[1]),
    ]
    for load in loads:
        load.start()

    barrier = pltpu.get_barrier_semaphore()
    for step in range(1, 16):
        pl.semaphore_signal(
            barrier, inc=1, device_id=place((blk + step) % 16, grp), device_id_type=MESH
        )
    pl.semaphore_signal(barrier, inc=1, device_id=place(blk, other_core), device_id_type=MESH)

    @pl.when(z > 0)
    def _():
        pl.semaphore_signal(barrier, inc=1, device_id=place(blk, w_target), device_id_type=MESH)
        pl.semaphore_signal(barrier, inc=1, device_id=place(blk, w_source), device_id_type=MESH)

    pl.semaphore_wait(barrier, jnp.where(z > 0, 18, 16))

    def remote(src, dst, send, recv, b, g):
        return pltpu.make_async_remote_copy(
            src_ref=src, dst_ref=dst, send_sem=send, recv_sem=recv,
            device_id=place(b, g), device_id_type=MESH,
        )

    def low_copy(event, src):
        return remote(src, from_low.at[event], low_send.at[event], low_recv.at[event], z_up, grp)

    def high_copy(event, src):
        return remote(
            src, from_high.at[event], high_send.at[event], high_recv.at[event], z_down, grp
        )

    for load in loads:
        load.wait()
    low_copy(0, from_low.at[7]).start()
    high_copy(0, from_high.at[7]).start()
    low_copy(1, from_high.at[7]).start()
    high_copy(1, from_low.at[7]).start()
    w_copy = remote(w_ref, w_pair.at[core], w_send, w_recv, blk, w_target)

    @pl.when(z > 0)
    def _():
        w_copy.start()

    @pl.when(z == 0)
    def _():
        w_pair[core] = w_ref[...]

    def arrive(event):
        low_copy(event, from_low.at[event]).wait_recv()

        @pl.when(event <= 4)
        def _():
            low_copy(event + 2, from_low.at[event]).start()

        high_copy(event, from_high.at[event]).wait_recv()

        @pl.when(event <= 4)
        def _():
            high_copy(event + 2, from_high.at[event]).start()

    arrive(0)
    arrive(1)

    @pl.when(z > 0)
    def _():
        w_copy.wait_recv()

    core_copy = remote(w_pair.at[core], w_pair.at[core], core_send, core_recv, blk, other_core)
    core_copy.start()
    core_back = remote(
        w_pair.at[1 - core], w_pair.at[1 - core], core_send, core_recv, blk, other_core
    )
    core_back.wait_recv()

    scale = jnp.where(
        lax.broadcasted_iota(jnp.int32, (1, 192), 1) < 64, math.log2(math.e) / 8.0, 1.0
    )
    ones = jnp.ones((rows, 64), jnp.bfloat16)

    def sources(slot):
        own = slot == 7
        last = slot == 6
        low_z = jnp.where(own, z, jnp.where(last, z + 4, z + 7 - slot // 2)) % 8
        high_z = jnp.where(own, z, jnp.where(last, z + 4, z + 1 + slot // 2)) % 8
        odd = slot % 2
        low_half = jnp.where(own, 0, odd)
        high_half = jnp.where(own, 1, 1 - odd)
        low_row = low_z * (2 * rows) + low_half * half
        high_row = high_z * (2 * rows) + high_half * half
        return low_row, high_row

    def swap_copy(slot, side, row):
        return remote(
            stage.at[slot, side], qkv.at[pl.ds(row, half)], swap_send.at[slot, side],
            swap_recv.at[slot, side], partner, grp,
        )

    def project(index, carry):
        slot = (index + 7) % 8

        @pl.when(index >= 3)
        def _():
            arrive(index - 1)

        low_row, high_row = sources(slot)
        low_at = pl.multiple_of(low_row + y_low * rows, half)
        high_at = pl.multiple_of(high_row + y_low * rows, half)
        frames = jnp.concatenate([from_low[slot], from_high[slot]], axis=0).astype(jnp.float32)
        normed = normalize(frames, gain_ref[...]).astype(jnp.bfloat16)

        def head_rows(which):
            product = jnp.dot(normed, w_pair[which], preferred_element_type=jnp.float32) * scale
            return jnp.concatenate([product.astype(jnp.bfloat16), ones], axis=1)

        away = head_rows(1 - y_low)
        stage[slot, 0] = away[:half]
        stage[slot, 1] = away[half:]
        swap_copy(slot, 0, low_at).start()
        swap_copy(slot, 1, high_at).start()
        home = head_rows(y_low)
        qkv[pl.ds(low_at, half)] = home[:half]
        qkv[pl.ds(high_at, half)] = home[half:]
        return carry

    lax.fori_loop(0, 8, project, 0)

    lane = lax.broadcasted_iota(jnp.int32, (1, 128), 1)
    begin = jnp.zeros((1, 128), jnp.int32)
    end = jnp.zeros((1, 128), jnp.int32)
    start = jnp.int32(0)
    for c in range(8):
        stop = start + utt_ref[c]
        begin = jnp.where(lane == 64 + c, start, begin)
        end = jnp.where(lane == 64 + c, stop, end)
        start = stop

    def arrange(index, carry):
        slot = (index + 7) % 8
        low_row, high_row = sources(slot)
        for side, row in ((0, low_row), (1, high_row)):
            theirs = pl.multiple_of(row + (1 - y_low) * rows, half)
            swap_copy(slot, side, theirs).wait_recv()
            mine = pl.multiple_of(row + y_low * rows, half)
            for at in (theirs, mine):
                both = qkv[pl.ds(at, half), :128]
                position = (
                    lax.broadcasted_iota(jnp.int32, (half, 128), 0) + (at + grp * (16 * rows))
                )
                member = (position >= begin) & (position < end)
                inside = member.astype(jnp.float32)
                query_mark = jnp.where(lane < 72, (1.0 - inside) * big_negative, 0.0)
                whole = both.astype(jnp.float32)
                query[pl.ds(at, half)] = jnp.where(lane < 64, whole, query_mark).astype(
                    jnp.bfloat16
                )
                keys[pl.ds(at, half)] = jnp.where(
                    lane < 64, pltpu.roll(whole, 64, 1), inside
                ).astype(jnp.bfloat16)
        return carry

    lax.fori_loop(0, 8, arrange, 0)

    window = 16 * rows
    key_block = 512
    key_steps = window // key_block

    def score_block(block, step):
        queries = query[pl.ds(pl.multiple_of(block * rows, rows), rows)]
        return lax.dot_general(
            queries, keys[step * key_block : (step + 1) * key_block],
            (((1,), (1,)), ((), ())), preferred_element_type=jnp.float32,
        )

    def lane_max(best, block_scores):
        for piece in range(key_block // 128):
            best = jnp.maximum(best, block_scores[:, piece * 128 : (piece + 1) * 128])
        return best

    def first_pass(block, buffer):
        best = jnp.full((rows, 128), -jnp.inf, jnp.float32)
        for step in range(key_steps):
            got = score_block(block, step)
            scores[buffer, :, step * key_block : (step + 1) * key_block] = got
            best = lane_max(best, got)
        return jnp.max(best, axis=1, keepdims=True)

    def target_of(index):
        return (blk + 1 + index) % 16

    def attend(index, row_max):
        block = target_of(index)
        following = target_of(index + 1)
        buffer = index % 2
        total = jnp.zeros((rows, 128), jnp.float32)
        best = jnp.full((rows, 128), -jnp.inf, jnp.float32)
        for step in range(key_steps):
            span = slice(step * key_block, (step + 1) * key_block)
            weights = jnp.exp2(scores[buffer, :, span] - row_max).astype(jnp.bfloat16)
            got = score_block(following, step)
            scores[1 - buffer, :, span] = got
            best = lane_max(best, got)
            total = total + jnp.dot(
                weights, qkv[span, 128:], preferred_element_type=jnp.float32
            )
        mixed = total / pltpu.roll(total, 64, 1)
        packed = jnp.where(lane < 64, mixed[:half], pltpu.roll(mixed[half:], 64, 1)).astype(
            jnp.bfloat16
        )

        @pl.when(index < 15)
        def _():
            out_stage[index] = packed
            out_copy(index, block).start()

        @pl.when(index == 15)
        def _():
            att_ref[my_head] = packed

        return jnp.max(best, axis=1, keepdims=True)

    def out_copy(index, block):
        return remote(
            out_stage.at[index], att_ref.at[my_head], out_send.at[index], out_recv.at[index],
            block, grp,
        )

    lax.fori_loop(0, 16, attend, first_pass(target_of(0), 0))

    def collect(index, carry):
        from_blk = (blk + 15 - index) % 16
        from_z = from_blk // 2
        head = (
            ((x + from_z % 4) % 4) * 4 + ((y_high + from_z // 4) % 2) * 2 + from_blk % 2
        )
        got = remote(
            out_stage.at[index], att_ref.at[head], out_send.at[index], out_recv.at[index],
            from_blk, grp,
        )
        got.wait_recv()
        got.wait_send()
        return carry

    lax.fori_loop(0, 15, collect, 0)

    for event in range(7):
        low_copy(event, from_low.at[event]).wait_send()
        high_copy(event, from_high.at[event]).wait_send()
    for slot in range(8):
        for side in range(2):
            swap_copy(slot, side, 0).wait_send()
    core_copy.wait_send()

    @pl.when(z > 0)
    def _():
        w_copy.wait_send()


def attend_all(frames, utt_lengths, attn_gain, w_qkv):
    rows, width = frames.shape
    half = rows // 2
    window = rows * 16
    vmem = pl.BlockSpec(memory_space=pltpu.VMEM)
    dma = pltpu.SemaphoreType.DMA
    return pl.pallas_call(
        attention_kernel,
        out_shape=jax.ShapeDtypeStruct((HEADS, half, 128), jnp.bfloat16),
        in_specs=[
            pl.BlockSpec(memory_space=pltpu.SMEM),
            pl.BlockSpec(memory_space=pl.ANY),
            vmem,
            vmem,
        ],
        out_specs=vmem,
        scratch_shapes=[
            pltpu.VMEM((8, half, width), jnp.bfloat16),
            pltpu.VMEM((8, half, width), jnp.bfloat16),
            pltpu.VMEM((2, width, 192), jnp.bfloat16),
            pltpu.VMEM((8, 2, half, 256), jnp.bfloat16),
            pltpu.VMEM((window, 256), jnp.bfloat16),
            pltpu.VMEM((window, 128), jnp.bfloat16),
            pltpu.VMEM((window, 128), jnp.bfloat16),
            pltpu.VMEM((2, rows, window), jnp.float32),
            pltpu.VMEM((15, half, 128), jnp.bfloat16),
            dma((2,)),
            dma((7,)), dma((7,)), dma((7,)), dma((7,)),
            dma, dma, dma, dma,
            dma((8, 2)), dma((8, 2)),
            dma((15,)), dma((15,)),
        ],
        compiler_params=pltpu.CompilerParams(
            collective_id=0, has_side_effects=True, vmem_limit_bytes=48 * 1024 * 1024
        ),
    )(utt_lengths, frames, attn_gain.reshape(1, width), w_qkv)


def padded_2(block, sides, width, periodic):
    for axis, dim in sides:
        count = lax.axis_size(axis)
        forward = [(i, i + 1) for i in range(count - 1)]
        if periodic:
            forward.append((count - 1, 0))
        backward = [(target, source) for source, target in forward]
        low = lax.ppermute(
            lax.slice_in_dim(block, block.shape[dim] - width, None, axis=dim), axis, forward
        )
        high = lax.ppermute(lax.slice_in_dim(block, 0, width, axis=dim), axis, backward)
        block = jnp.concatenate([low, block, high], axis=dim)
    return block


def body(
    frames, utt_lengths, attn_gain, w_qkv, w_out, conv_gain, w_glu, w_depth, depth_gain, w_proj
):
    frame_rows = frames.shape[1]
    width = frames.shape[2]
    kernel_half = (w_depth.shape[0] - 1) // 2
    blocks = lax.axis_size("blk")
    block_index = lax.axis_index("blk")
    group_index = lax.axis_index("grp")
    window_start = group_index * frame_rows * blocks
    first_frame = window_start + block_index * frame_rows
    local_frames = frames[0]
    local_float = local_frames.astype(jnp.float32)
    local_seg = segment_of(utt_lengths, first_frame + jnp.arange(frame_rows, dtype=jnp.int32))
    packed = attend_all(local_frames, utt_lengths, attn_gain, w_qkv)
    attended = jnp.transpose(
        packed.reshape(HEADS, frame_rows // 2, 2, width // HEADS), (2, 1, 0, 3)
    ).reshape(frame_rows, width)
    residual = (local_float + jnp.dot(attended, w_out, preferred_element_type=jnp.float32)).astype(
        jnp.bfloat16
    )
    residual = lax.optimization_barrier(residual)
    conv_in = normalize(residual.astype(jnp.float32), conv_gain).astype(jnp.bfloat16)
    projected = jnp.dot(conv_in, w_glu, preferred_element_type=jnp.float32)
    gated = (projected[:, :width] * jax.nn.sigmoid(projected[:, width:])).astype(jnp.bfloat16)
    gated = lax.optimization_barrier(gated)
    padded = padded_2(gated, (("blk", 0),), kernel_half, True)
    left_rim = padded[:kernel_half]
    right_rim = padded[frame_rows + kernel_half :]
    outer_rims = padded_2(jnp.stack([right_rim, left_rim]), (("grp", 0),), 1, False)
    left_edge = jnp.where(block_index == 0, outer_rims[0], left_rim)
    right_edge = jnp.where(block_index == blocks - 1, outer_rims[3], right_rim)
    extended = jnp.concatenate([left_edge, gated, right_edge], axis=0).astype(jnp.float32)
    extended_seg = segment_of(
        utt_lengths,
        first_frame - kernel_half + jnp.arange(frame_rows + 2 * kernel_half, dtype=jnp.int32),
    )
    mixed_conv = jnp.zeros((frame_rows, width), jnp.float32)
    for offset in range(2 * kernel_half + 1):
        same_seg = (extended_seg[offset : offset + frame_rows] == local_seg)[:, None]
        mixed_conv = mixed_conv + jnp.where(
            same_seg, extended[offset : offset + frame_rows] * w_depth[offset], 0.0
        )
    normed_conv = normalize(mixed_conv, depth_gain)
    activated = (normed_conv * jax.nn.sigmoid(normed_conv)).astype(jnp.bfloat16)
    result = (
        residual.astype(jnp.float32)
        + jnp.dot(activated, w_proj, preferred_element_type=jnp.float32)
    ).astype(jnp.bfloat16)
    return result[None]


def solution(mesh):
    in_specs = (P("grp", "blk", None), P(), P(), P(None, "grp"), P(), P(), P(), P(), P(), P())
    out_specs = P("grp", "blk", None)
    return jax.shard_map(body, mesh=mesh, in_specs=in_specs, out_specs=out_specs, check_vma=False)
```

```python
import functools
import math

import jax
import jax.numpy as jnp
from jax import lax
from jax.experimental import pallas as pl
from jax.experimental.pallas import tpu as pltpu
from jax.sharding import PartitionSpec as P

HEADS = 16
SETS = 8
HALO = 16
MESH = pl.DeviceIdType.MESH

epsilon = 1e-05
big_negative = -1e30
lowest = -2e38


def normalize(values, row_gain):
    center = values - jnp.mean(values, axis=-1, keepdims=True)
    spread = jnp.mean(center * center, axis=-1, keepdims=True)
    return center * lax.rsqrt(spread + epsilon) * row_gain


def mixing_kernel(
    utt_hbm, frames_hbm, gain_hbm, w_hbm, w_out_hbm, conv_gain_hbm, w_glu_hbm,
    gated_ref, residual_ref,
    utt, gain, conv_gain, w_mine, w_out, w_glu,
    from_low, from_high, w_pair, stage, qkv, query, keys, peak, mix, buf_a, buf_b,
    out_stage, att, attended,
    load_sem, low_send, low_recv, high_send, high_recv, w_send, w_recv, core_send, core_recv,
    swap_send, swap_recv, out_send, out_recv, halo_send, halo_recv,
):
    half = from_low.shape[1]
    rows = 2 * half
    blk = lax.axis_index("blk")
    grp = lax.axis_index("grp")
    z, y_low = blk // 2, blk % 2
    x, y_high, core = grp // 4, (grp // 2) % 2, grp % 2
    dx, dy = z % 4, z // 4
    head_x, head_y = (x + dx) % 4, (y_high + dy) % 2
    w_source = head_x * 4 + head_y * 2 + core
    w_target = ((x + 4 - dx) % 4) * 4 + head_y * 2 + core
    my_head = head_x * 4 + head_y * 2 + y_low
    other_core = grp + 1 - 2 * core
    partner = blk + 1 - 2 * y_low
    z_up = (blk + 2) % 16
    z_down = (blk + 14) % 16
    left = ((blk + 15) % 16, (grp + jnp.where(blk == 0, 15, 0)) % 16)
    right = ((blk + 1) % 16, (grp + jnp.where(blk == 15, 1, 0)) % 16)

    def place(b, g):
        return {"blk": b, "grp": g}

    def load(index, src, dst):
        return pltpu.make_async_copy(src, dst, load_sem.at[index])

    loads = [
        load(0, frames_hbm.at[pl.ds(0, half)], from_low.at[7]),
        load(1, frames_hbm.at[pl.ds(half, half)], from_high.at[7]),
        load(2, w_hbm, w_mine),
        load(3, gain_hbm, gain),
        load(4, utt_hbm, utt),
        load(5, conv_gain_hbm, conv_gain),
        load(6, w_out_hbm, w_out),
        load(7, w_glu_hbm, w_glu),
    ]
    for item in loads:
        item.start()

    barrier = pltpu.get_barrier_semaphore()

    def greet(b, g):
        pl.semaphore_signal(barrier, inc=1, device_id=place(b, g), device_id_type=MESH)

    for step in range(1, 16):
        greet((blk + step) % 16, grp)
    greet(blk, other_core)
    greet(*left)
    greet(*right)

    @pl.when(z > 0)
    def _():
        greet(blk, w_target)
        greet(blk, w_source)

    pl.semaphore_wait(barrier, jnp.where(z > 0, 20, 18))

    def remote(src, dst, send, recv, b, g):
        return pltpu.make_async_remote_copy(
            src_ref=src, dst_ref=dst, send_sem=send, recv_sem=recv,
            device_id=place(b, g), device_id_type=MESH,
        )

    def low_copy(event, src):
        return remote(src, from_low.at[event], low_send.at[event], low_recv.at[event], z_up, grp)

    def high_copy(event, src):
        return remote(
            src, from_high.at[event], high_send.at[event], high_recv.at[event], z_down, grp
        )

    loads[0].wait()
    loads[1].wait()
    low_copy(0, from_low.at[7]).start()
    high_copy(0, from_high.at[7]).start()
    low_copy(1, from_high.at[7]).start()
    high_copy(1, from_low.at[7]).start()
    loads[2].wait()
    w_copy = remote(w_mine, w_pair.at[core], w_send, w_recv, blk, w_target)

    @pl.when(z > 0)
    def _():
        w_copy.start()

    @pl.when(z == 0)
    def _():
        w_pair[core] = w_mine[...]

    loads[3].wait()
    loads[4].wait()

    def arrive(event):
        low_copy(event, from_low.at[event]).wait_recv()

        @pl.when(event <= 4)
        def _():
            low_copy(event + 2, from_low.at[event]).start()

        high_copy(event, from_high.at[event]).wait_recv()

        @pl.when(event <= 4)
        def _():
            high_copy(event + 2, from_high.at[event]).start()

    arrive(0)
    arrive(1)

    @pl.when(z > 0)
    def _():
        w_copy.wait_recv()

    core_copy = remote(w_pair.at[core], w_pair.at[core], core_send, core_recv, blk, other_core)
    core_copy.start()
    core_back = remote(
        w_pair.at[1 - core], w_pair.at[1 - core], core_send, core_recv, blk, other_core
    )
    core_back.wait_recv()

    lane = lax.broadcasted_iota(jnp.int32, (1, 128), 1)
    begin = jnp.zeros((1, 128), jnp.int32)
    end = jnp.zeros((1, 128), jnp.int32)
    start = jnp.int32(0)
    for c in range(8):
        stop = start + utt[c]
        begin = jnp.where(lane == 64 + c, start, begin)
        end = jnp.where(lane == 64 + c, stop, end)
        start = stop
    scale = jnp.where(
        lax.broadcasted_iota(jnp.int32, (1, 192), 1) < 64, math.log2(math.e) / 8.0, 1.0
    )
    ones = jnp.ones((rows, 64), jnp.bfloat16)

    def chunk_of(s, side):
        event = s + 7
        odd = event % 2
        away = jnp.where(s == 0, 0, jnp.where(s == 7, 4, (s + 1) // 2))
        if side == 0:
            return (z + 8 - away) % 8, jnp.where(s == 0, 0, odd)
        return (z + away) % 8, jnp.where(s == 0, 1, 1 - odd)

    def swap_copy(s, side):
        return remote(
            stage.at[s, side], qkv.at[s, pl.ds(rows + side * half, half)],
            swap_send.at[s, side], swap_recv.at[s, side], partner, grp,
        )

    def project(s):
        slot = (s + 7) % 8
        frames = jnp.concatenate([from_low[slot], from_high[slot]], axis=0).astype(jnp.float32)
        normed = normalize(frames, gain[...]).astype(jnp.bfloat16)

        def head_rows(which):
            product = lax.dot_general(
                normed, w_pair[which], (((1,), (1,)), ((), ())),
                preferred_element_type=jnp.float32,
            ) * scale
            return jnp.concatenate([product.astype(jnp.bfloat16), ones], axis=1)

        theirs = head_rows(1 - y_low)
        stage[s, 0] = theirs[:half]
        stage[s, 1] = theirs[half:]
        swap_copy(s, 0).start()
        swap_copy(s, 1).start()
        qkv[s, :rows] = head_rows(y_low)

    def arrange(s):
        swap_copy(s, 0).wait_recv()
        swap_copy(s, 1).wait_recv()
        for piece in range(4):
            from_z, from_half = chunk_of(s, piece % 2)
            plane = y_low if piece < 2 else 1 - y_low
            first = grp * (16 * rows) + (from_z * 2 + plane) * rows + from_half * half
            span = slice(piece * half, (piece + 1) * half)
            whole = qkv[s, span, :128].astype(jnp.float32)
            position = lax.broadcasted_iota(jnp.int32, (half, 128), 0) + first
            inside = ((position >= begin) & (position < end)).astype(jnp.float32)
            query_mark = jnp.where(lane < 72, (1.0 - inside) * big_negative, 0.0)
            query[s, span] = jnp.where(lane < 64, whole, query_mark).astype(jnp.bfloat16)
            keys[s, span] = jnp.where(lane < 64, pltpu.roll(whole, 64, 1), inside).astype(
                jnp.bfloat16
            )
        peak[s] = jnp.full((2 * rows, 128), lowest, jnp.float32)
        mix[s] = jnp.zeros((2 * rows, 128), jnp.float32)

    def score(q, k):
        return lax.dot_general(
            query[q], keys[k], (((1,), (1,)), ((), ())), preferred_element_type=jnp.float32
        )

    def absorb(q, k, buf):
        tiles = [buf[:, t * 128 : (t + 1) * 128] for t in range(2 * rows // 128)]
        old = peak[q]
        new = jnp.maximum(
            old, jnp.max(functools.reduce(jnp.maximum, tiles), axis=1, keepdims=True)
        )
        weights = jnp.concatenate(
            [jnp.exp2(tile - new).astype(jnp.bfloat16) for tile in tiles], axis=1
        )
        mix[q] = mix[q] * jnp.exp2(old - new) + jnp.dot(
            weights, qkv[k, :, 128:], preferred_element_type=jnp.float32
        )
        peak[q] = new

    def pair(s, p):
        return jnp.where(p <= s, s, 2 * s - p), jnp.where(p <= s, p, s)

    def two_pairs(s, t):
        q0, k0 = pair(s, 2 * t)
        q1, k1 = pair(s, 2 * t + 1)
        q2, k2 = pair(s, 2 * t + 2)
        buf_b[...] = score(q1, k1)
        absorb(q0, k0, buf_a)
        buf_a[...] = score(q2, k2)
        absorb(q1, k1, buf_b)
        return q0, q1

    def first_score(s):
        buf_a[...] = score(s, 0)

    def attend(s):
        first_score(s)

        def both(t, carry):
            two_pairs(s, t)
            return carry

        lax.fori_loop(0, s, both, 0)
        absorb(*pair(s, 2 * s), buf_a)

    def step(s, carry):
        @pl.when(s >= 3)
        def _():
            arrive(s - 1)

        project(s)

        @pl.when(s >= 1)
        def _():
            arrange(s - 1)
            attend(s - 1)

        return carry

    lax.fori_loop(0, SETS, step, 0)

    def out_copy(s, piece):
        to_z, to_half = chunk_of(s, piece % 2)
        plane = y_low if piece < 2 else 1 - y_low
        return remote(
            out_stage.at[s, piece], att.at[my_head, to_half], out_send.at[s, piece],
            out_recv.at[s, piece], to_z * 2 + plane, grp,
        )

    def finish(s):
        total = mix[s]
        mixed = total / pltpu.roll(total, 64, 1)
        turned = pltpu.roll(mixed, 64, 1)
        quarter = half // 2
        packed = [
            jnp.where(
                lane < 64, mixed[piece * half : piece * half + quarter],
                turned[piece * half + quarter : (piece + 1) * half],
            ).astype(jnp.bfloat16)
            for piece in range(4)
        ]

        @pl.when(s > 0)
        def _():
            for piece in range(2):
                out_stage[s, piece] = packed[piece]
                out_copy(s, piece).start()

        @pl.when(s == 0)
        def _():
            att[my_head, 0] = packed[0]
            att[my_head, 1] = packed[1]

        for piece in range(2, 4):
            out_stage[s, piece] = packed[piece]
            out_copy(s, piece).start()

    last = SETS - 1
    arrange(last)
    first_score(last)

    def gather_last(t, carry):
        two_pairs(last, t)
        return carry

    lax.fori_loop(0, 4, gather_last, 0)
    finish(last)

    def release(t, carry):
        q0, q1 = two_pairs(last, t)
        finish(q0)
        finish(q1)
        return carry

    lax.fori_loop(4, 7, release, 0)
    absorb(*pair(last, 2 * last), buf_a)
    finish(0)
    loads[5].wait()
    loads[6].wait()
    loads[7].wait()

    def collect(s, carry):
        for piece in range(4):
            plane = y_low if piece < 2 else 1 - y_low
            from_z, _ = chunk_of(s, 1 - piece % 2)
            _, at_half = chunk_of(s, piece % 2)
            head = ((x + from_z % 4) % 4) * 4 + ((y_high + from_z // 4) % 2) * 2 + plane
            got = remote(
                out_stage.at[s, piece], att.at[head, at_half], out_send.at[s, piece],
                out_recv.at[s, piece], from_z * 2 + plane, grp,
            )
            if piece < 2:
                @pl.when(s > 0)
                def _():
                    got.wait_recv()
                    got.wait_send()
            else:
                got.wait_recv()
                got.wait_send()
        return carry

    lax.fori_loop(0, SETS, collect, 0)

    quarter = half // 2
    for side in range(2):
        for two in range(HEADS // 2):
            one = att[2 * two, side].astype(jnp.float32)
            other = att[2 * two + 1, side].astype(jnp.float32)
            top = jnp.where(lane < 64, one, pltpu.roll(other, 64, 1))
            low = jnp.where(lane < 64, pltpu.roll(one, 64, 1), other)
            span = slice(two * 128, (two + 1) * 128)
            at = side * half
            attended[at : at + quarter, span] = top.astype(jnp.bfloat16)
            attended[at + quarter : at + half, span] = low.astype(jnp.bfloat16)

    frames = jnp.concatenate([from_low[7], from_high[7]], axis=0).astype(jnp.float32)
    residual = (
        frames + jnp.dot(attended[...], w_out[...], preferred_element_type=jnp.float32)
    ).astype(jnp.bfloat16)
    residual_ref[...] = residual
    conv_in = normalize(residual.astype(jnp.float32), conv_gain[...]).astype(jnp.bfloat16)
    width = residual.shape[1]
    for column in range(0, width, 256):
        values = jnp.dot(
            conv_in, w_glu[:, column : column + 256], preferred_element_type=jnp.float32
        )
        gates = jnp.dot(
            conv_in, w_glu[:, width + column : width + column + 256],
            preferred_element_type=jnp.float32,
        )
        gated_ref[HALO : HALO + rows, column : column + 256] = (
            values * jax.nn.sigmoid(gates)
        ).astype(jnp.bfloat16)

    to_left = remote(
        gated_ref.at[pl.ds(HALO, HALO)], gated_ref.at[pl.ds(HALO + rows, HALO)],
        halo_send.at[0], halo_recv.at[0], *left,
    )
    to_right = remote(
        gated_ref.at[pl.ds(rows, HALO)], gated_ref.at[pl.ds(0, HALO)],
        halo_send.at[1], halo_recv.at[1], *right,
    )
    to_left.start()
    to_right.start()

    for event in range(7):
        low_copy(event, from_low.at[event]).wait_send()
        high_copy(event, from_high.at[event]).wait_send()
    for s in range(SETS):
        for side in range(2):
            swap_copy(s, side).wait_send()
    core_copy.wait_send()

    @pl.when(z > 0)
    def _():
        w_copy.wait_send()

    to_left.wait()
    to_right.wait()


def mix_all(frames, utt_lengths, attn_gain, w_qkv, w_out, conv_gain, w_glu):
    rows, width = frames.shape
    half = rows // 2
    hbm = pl.BlockSpec(memory_space=pltpu.HBM)
    vmem = pl.BlockSpec(memory_space=pltpu.VMEM)
    dma = pltpu.SemaphoreType.DMA
    bf16, f32 = jnp.bfloat16, jnp.float32
    return pl.pallas_call(
        mixing_kernel,
        out_shape=(
            jax.ShapeDtypeStruct((rows + 2 * HALO, width), bf16),
            jax.ShapeDtypeStruct((rows, width), bf16),
        ),
        in_specs=[hbm] * 7,
        out_specs=(vmem, vmem),
        scratch_shapes=[
            pltpu.SMEM((8,), jnp.int32),
            pltpu.VMEM((1, width), f32),
            pltpu.VMEM((1, width), f32),
            pltpu.VMEM((192, width), bf16),
            pltpu.VMEM((width, width), bf16),
            pltpu.VMEM((width, 2 * width), bf16),
            pltpu.VMEM((8, half, width), bf16),
            pltpu.VMEM((8, half, width), bf16),
            pltpu.VMEM((2, 192, width), bf16),
            pltpu.VMEM((SETS, 2, half, 256), bf16),
            pltpu.VMEM((SETS, 2 * rows, 256), bf16),
            pltpu.VMEM((SETS, 2 * rows, 128), bf16),
            pltpu.VMEM((SETS, 2 * rows, 128), bf16),
            pltpu.VMEM((SETS, 2 * rows, 128), f32),
            pltpu.VMEM((SETS, 2 * rows, 128), f32),
            pltpu.VMEM((2 * rows, 2 * rows), f32),
            pltpu.VMEM((2 * rows, 2 * rows), f32),
            pltpu.VMEM((SETS, 4, half // 2, 128), bf16),
            pltpu.VMEM((HEADS, 2, half // 2, 128), bf16),
            pltpu.VMEM((rows, width), bf16),
            dma((8,)),
            dma((7,)), dma((7,)), dma((7,)), dma((7,)),
            dma, dma, dma, dma,
            dma((SETS, 2)), dma((SETS, 2)),
            dma((SETS, 4)), dma((SETS, 4)),
            dma((2,)), dma((2,)),
        ],
        compiler_params=pltpu.CompilerParams(
            collective_id=0, has_side_effects=True, vmem_limit_bytes=44 * 1024 * 1024
        ),
    )(
        utt_lengths, frames, attn_gain.reshape(1, width), w_qkv.T, w_out,
        conv_gain.reshape(1, width), w_glu,
    )


def conv_kernel(
    utt, gated_ref, residual_ref, w_depth_ref, gain_ref, w_proj_ref,
    out_ref,
    tall, mixed, activated,
):
    rows, width = residual_ref.shape
    taps = w_depth_ref.shape[0]
    reach = taps // 2
    columns = width // 128
    first = (lax.axis_index("grp") * 16 + lax.axis_index("blk")) * rows
    for c in range(columns):
        tall[c] = gated_ref[:, c * 128 : (c + 1) * 128].astype(jnp.float32)

    block = 64

    def convolve(r, carry):
        base = pl.multiple_of(r * block, block)
        position = first + base
        start = jnp.int32(0)
        low, high = jnp.int32(0), jnp.int32(0)
        for c in range(8):
            stop = start + utt[c]
            low = jnp.where(start <= position, start, low)
            high = jnp.where(start <= position, stop, high)
            start = stop
        whole = (low <= position - reach) & (high >= position + block + reach)

        def taps_of(mask):
            def column(c, carry):
                total = jnp.zeros((block, 128), jnp.float32)
                for t in range(taps):
                    term = (
                        tall[c, pl.ds(base + (HALO - reach + t), block)]
                        * w_depth_ref[t : t + 1, pl.ds(pl.multiple_of(c * 128, 128), 128)]
                    )
                    if mask is not None:
                        term = mask(t, term)
                    total = total + term
                mixed[c, pl.ds(base, block)] = total
                return carry

            lax.fori_loop(0, columns, column, 0)

        @pl.when(whole)
        def _():
            taps_of(None)

        @pl.when(jnp.logical_not(whole))
        def _():
            at = lax.broadcasted_iota(jnp.int32, (block, 128), 0) + position
            begin = jnp.zeros((block, 128), jnp.int32)
            end = jnp.zeros((block, 128), jnp.int32)
            start = jnp.int32(0)
            for c in range(8):
                stop = start + utt[c]
                begin = jnp.where(at >= start, start, begin)
                end = jnp.where(at >= start, stop, end)
                start = stop
            first_tap = begin - at + reach
            last_tap = end - at + reach
            taps_of(lambda t, term: jnp.where((first_tap <= t) & (last_tap > t), term, 0.0))

        pieces = [mixed[c, pl.ds(base, block)] for c in range(columns)]
        mean = jnp.sum(functools.reduce(jnp.add, pieces), axis=1, keepdims=True) / width
        pieces = [piece - mean for piece in pieces]
        spread = (
            jnp.sum(functools.reduce(jnp.add, [p * p for p in pieces]), axis=1, keepdims=True)
            / width
        )
        factor = lax.rsqrt(spread + epsilon)
        for c in range(columns):
            span = slice(c * 128, (c + 1) * 128)
            value = pieces[c] * factor * gain_ref[:, span]
            activated[pl.ds(base, block), span] = (value * jax.nn.sigmoid(value)).astype(
                jnp.bfloat16
            )
        return carry

    lax.fori_loop(0, rows // block, convolve, 0)
    for column in range(0, width, 256):
        span = slice(column, column + 256)
        out_ref[:, span] = (
            residual_ref[:, span].astype(jnp.float32)
            + jnp.dot(activated[...], w_proj_ref[:, span], preferred_element_type=jnp.float32)
        ).astype(jnp.bfloat16)


def convolve_all(utt_lengths, gated, residual, w_depth, depth_gain, w_proj):
    rows, width = residual.shape
    vmem = pl.BlockSpec(memory_space=pltpu.VMEM)
    return pl.pallas_call(
        conv_kernel,
        out_shape=jax.ShapeDtypeStruct((rows, width), jnp.bfloat16),
        in_specs=[pl.BlockSpec(memory_space=pltpu.SMEM)] + [vmem] * 5,
        out_specs=vmem,
        scratch_shapes=[
            pltpu.VMEM((width // 128, rows + 2 * HALO, 128), jnp.float32),
            pltpu.VMEM((width // 128, rows, 128), jnp.float32),
            pltpu.VMEM((rows, width), jnp.bfloat16),
        ],
        compiler_params=pltpu.CompilerParams(vmem_limit_bytes=24 * 1024 * 1024),
    )(utt_lengths, gated, residual, w_depth, depth_gain.reshape(1, width), w_proj)


def body(
    frames, utt_lengths, attn_gain, w_qkv, w_out, conv_gain, w_glu, w_depth, depth_gain, w_proj
):
    gated, residual = mix_all(
        frames[0], utt_lengths, attn_gain, w_qkv, w_out, conv_gain, w_glu
    )
    return convolve_all(utt_lengths, gated, residual, w_depth, depth_gain, w_proj)[None]


def solution(mesh):
    in_specs = (P("grp", "blk", None), P(), P(), P(None, "grp"), P(), P(), P(), P(), P(), P())
    out_specs = P("grp", "blk", None)
    return jax.shard_map(body, mesh=mesh, in_specs=in_specs, out_specs=out_specs, check_vma=False)
```

```python
import functools
import math

import jax
import jax.numpy as jnp
from jax import lax
from jax.experimental import pallas as pl
from jax.experimental.pallas import tpu as pltpu
from jax.sharding import PartitionSpec as P

HEADS = 16
SETS = 8
HALO = 16
MESH = pl.DeviceIdType.MESH

epsilon = 1e-05
big_negative = -1e30
lowest = -2e38


def normalize(values, row_gain):
    center = values - jnp.mean(values, axis=-1, keepdims=True)
    spread = jnp.mean(center * center, axis=-1, keepdims=True)
    return center * lax.rsqrt(spread + epsilon) * row_gain


def mixing_kernel(
    utt_hbm, frames_hbm, gain_hbm, w_hbm, w_out_hbm, conv_gain_hbm, w_glu_hbm, w_depth_hbm,
    depth_gain_hbm, w_proj_hbm,
    out_ref,
    utt, gain, conv_gain, depth_gain, w_mine, w_out, w_glu, w_depth, w_proj,
    from_low, from_high, w_pair, stage, qkv, query, keys, peak, mix, buf_a, buf_b,
    out_stage, att, attended, residual, edge_out, edge_in, tall, valid, mixed,
    load_sem, low_send, low_recv, high_send, high_recv, w_send, w_recv, core_send, core_recv,
    swap_send, swap_recv, out_send, out_recv, halo_send, halo_recv,
):
    half = from_low.shape[1]
    rows = 2 * half
    blk = lax.axis_index("blk")
    grp = lax.axis_index("grp")
    z, y_low = blk // 2, blk % 2
    x, y_high, core = grp // 4, (grp // 2) % 2, grp % 2
    dx, dy = z % 4, z // 4
    head_x, head_y = (x + dx) % 4, (y_high + dy) % 2
    w_source = head_x * 4 + head_y * 2 + core
    w_target = ((x + 4 - dx) % 4) * 4 + head_y * 2 + core
    my_head = head_x * 4 + head_y * 2 + y_low
    other_core = grp + 1 - 2 * core
    partner = blk + 1 - 2 * y_low
    z_up = (blk + 2) % 16
    z_down = (blk + 14) % 16
    left = ((blk + 15) % 16, (grp + jnp.where(blk == 0, 15, 0)) % 16)
    right = ((blk + 1) % 16, (grp + jnp.where(blk == 15, 1, 0)) % 16)

    def place(b, g):
        return {"blk": b, "grp": g}

    def load(index, src, dst):
        return pltpu.make_async_copy(src, dst, load_sem.at[index])

    loads = [
        load(0, frames_hbm.at[pl.ds(0, half)], from_low.at[7]),
        load(1, frames_hbm.at[pl.ds(half, half)], from_high.at[7]),
        load(2, w_hbm, w_mine),
        load(3, gain_hbm, gain),
        load(4, utt_hbm, utt),
        load(5, conv_gain_hbm, conv_gain),
        load(6, w_out_hbm, w_out),
        load(7, w_glu_hbm, w_glu),
        load(8, w_depth_hbm, w_depth),
        load(9, depth_gain_hbm, depth_gain),
        load(10, w_proj_hbm, w_proj),
    ]
    for item in loads:
        item.start()

    barrier = pltpu.get_barrier_semaphore()

    def greet(b, g):
        pl.semaphore_signal(barrier, inc=1, device_id=place(b, g), device_id_type=MESH)

    for step in range(1, 16):
        greet((blk + step) % 16, grp)
    greet(blk, other_core)
    greet(*left)
    greet(*right)

    @pl.when(z > 0)
    def _():
        greet(blk, w_target)
        greet(blk, w_source)

    pl.semaphore_wait(barrier, jnp.where(z > 0, 20, 18))

    def remote(src, dst, send, recv, b, g):
        return pltpu.make_async_remote_copy(
            src_ref=src, dst_ref=dst, send_sem=send, recv_sem=recv,
            device_id=place(b, g), device_id_type=MESH,
        )

    def low_copy(event, src):
        return remote(src, from_low.at[event], low_send.at[event], low_recv.at[event], z_up, grp)

    def high_copy(event, src):
        return remote(
            src, from_high.at[event], high_send.at[event], high_recv.at[event], z_down, grp
        )

    loads[0].wait()
    loads[1].wait()
    low_copy(0, from_low.at[7]).start()
    high_copy(0, from_high.at[7]).start()
    low_copy(1, from_high.at[7]).start()
    high_copy(1, from_low.at[7]).start()
    loads[2].wait()
    w_copy = remote(w_mine, w_pair.at[core], w_send, w_recv, blk, w_target)

    @pl.when(z > 0)
    def _():
        w_copy.start()

    @pl.when(z == 0)
    def _():
        w_pair[core] = w_mine[...]

    loads[3].wait()
    loads[4].wait()

    def arrive(event):
        low_copy(event, from_low.at[event]).wait_recv()

        @pl.when(event <= 4)
        def _():
            low_copy(event + 2, from_low.at[event]).start()

        high_copy(event, from_high.at[event]).wait_recv()

        @pl.when(event <= 4)
        def _():
            high_copy(event + 2, from_high.at[event]).start()

    arrive(0)
    arrive(1)

    @pl.when(z > 0)
    def _():
        w_copy.wait_recv()

    core_copy = remote(w_pair.at[core], w_pair.at[core], core_send, core_recv, blk, other_core)
    core_copy.start()
    core_back = remote(
        w_pair.at[1 - core], w_pair.at[1 - core], core_send, core_recv, blk, other_core
    )
    core_back.wait_recv()

    lane = lax.broadcasted_iota(jnp.int32, (1, 128), 1)
    begin = jnp.zeros((1, 128), jnp.int32)
    end = jnp.zeros((1, 128), jnp.int32)
    start = jnp.int32(0)
    for c in range(8):
        stop = start + utt[c]
        begin = jnp.where(lane == 64 + c, start, begin)
        end = jnp.where(lane == 64 + c, stop, end)
        start = stop
    scale = jnp.where(
        lax.broadcasted_iota(jnp.int32, (1, 192), 1) < 64, math.log2(math.e) / 8.0, 1.0
    )
    ones = jnp.ones((rows, 64), jnp.bfloat16)

    def chunk_of(s, side):
        event = s + 7
        odd = event % 2
        away = jnp.where(s == 0, 0, jnp.where(s == 7, 4, (s + 1) // 2))
        if side == 0:
            return (z + 8 - away) % 8, jnp.where(s == 0, 0, odd)
        return (z + away) % 8, jnp.where(s == 0, 1, 1 - odd)

    def swap_copy(s, side):
        return remote(
            stage.at[s, side], qkv.at[s, pl.ds(rows + side * half, half)],
            swap_send.at[s, side], swap_recv.at[s, side], partner, grp,
        )

    def project(s):
        slot = (s + 7) % 8
        frames = jnp.concatenate([from_low[slot], from_high[slot]], axis=0).astype(jnp.float32)
        normed = normalize(frames, gain[...]).astype(jnp.bfloat16)

        def head_rows(which):
            product = lax.dot_general(
                normed, w_pair[which], (((1,), (1,)), ((), ())),
                preferred_element_type=jnp.float32,
            ) * scale
            return jnp.concatenate([product.astype(jnp.bfloat16), ones], axis=1)

        theirs = head_rows(1 - y_low)
        stage[s, 0] = theirs[:half]
        stage[s, 1] = theirs[half:]
        swap_copy(s, 0).start()
        swap_copy(s, 1).start()
        qkv[s, :rows] = head_rows(y_low)

    def arrange(s):
        swap_copy(s, 0).wait_recv()
        swap_copy(s, 1).wait_recv()
        for piece in range(4):
            from_z, from_half = chunk_of(s, piece % 2)
            plane = y_low if piece < 2 else 1 - y_low
            first = grp * (16 * rows) + (from_z * 2 + plane) * rows + from_half * half
            span = slice(piece * half, (piece + 1) * half)
            whole = qkv[s, span, :128].astype(jnp.float32)
            position = lax.broadcasted_iota(jnp.int32, (half, 128), 0) + first
            inside = ((position >= begin) & (position < end)).astype(jnp.float32)
            query_mark = jnp.where(lane < 72, (1.0 - inside) * big_negative, 0.0)
            query[s, span] = jnp.where(lane < 64, whole, query_mark).astype(jnp.bfloat16)
            keys[s, span] = jnp.where(lane < 64, pltpu.roll(whole, 64, 1), inside).astype(
                jnp.bfloat16
            )
        peak[s] = jnp.full((2 * rows, 128), lowest, jnp.float32)
        mix[s] = jnp.zeros((2 * rows, 128), jnp.float32)

    def score(q, k):
        return lax.dot_general(
            query[q], keys[k], (((1,), (1,)), ((), ())), preferred_element_type=jnp.float32
        )

    def absorb(q, k, buf):
        tiles = [buf[:, t * 128 : (t + 1) * 128] for t in range(2 * rows // 128)]
        old = peak[q]
        new = jnp.maximum(
            old, jnp.max(functools.reduce(jnp.maximum, tiles), axis=1, keepdims=True)
        )
        weights = jnp.concatenate(
            [jnp.exp2(tile - new).astype(jnp.bfloat16) for tile in tiles], axis=1
        )
        mix[q] = mix[q] * jnp.exp2(old - new) + jnp.dot(
            weights, qkv[k, :, 128:], preferred_element_type=jnp.float32
        )
        peak[q] = new

    def pair(s, p):
        return jnp.where(p <= s, s, 2 * s - p), jnp.where(p <= s, p, s)

    def two_pairs(order, s, t):
        q0, k0 = order(s, 2 * t)
        q1, k1 = order(s, 2 * t + 1)
        q2, k2 = order(s, 2 * t + 2)
        buf_b[...] = score(q1, k1)
        absorb(q0, k0, buf_a)
        buf_a[...] = score(q2, k2)
        absorb(q1, k1, buf_b)
        return q0, q1

    def attend(s):
        buf_a[...] = score(s, 0)

        def both(t, carry):
            two_pairs(pair, s, t)
            return carry

        lax.fori_loop(0, s, both, 0)
        absorb(*pair(s, 2 * s), buf_a)

    def step(s, carry):
        @pl.when(s >= 3)
        def _():
            arrive(s - 1)

        project(s)

        @pl.when(s >= 1)
        def _():
            arrange(s - 1)
            attend(s - 1)

        return carry

    lax.fori_loop(0, SETS, step, 0)

    def out_copy(s, piece):
        to_z, to_half = chunk_of(s, piece % 2)
        plane = y_low if piece < 2 else 1 - y_low
        return remote(
            out_stage.at[s, piece], att.at[my_head, to_half], out_send.at[s, piece],
            out_recv.at[s, piece], to_z * 2 + plane, grp,
        )

    def finish(s):
        total = mix[s]
        mixed = total / pltpu.roll(total, 64, 1)
        turned = pltpu.roll(mixed, 64, 1)
        quarter = half // 2
        packed = [
            jnp.where(
                lane < 64, mixed[piece * half : piece * half + quarter],
                turned[piece * half + quarter : (piece + 1) * half],
            ).astype(jnp.bfloat16)
            for piece in range(4)
        ]

        @pl.when(s > 0)
        def _():
            for piece in range(2):
                out_stage[s, piece] = packed[piece]
                out_copy(s, piece).start()

        @pl.when(s == 0)
        def _():
            att[my_head, 0] = packed[0]
            att[my_head, 1] = packed[1]

        for piece in range(2, 4):
            out_stage[s, piece] = packed[piece]
            out_copy(s, piece).start()

    last = SETS - 1

    def last_pair(s, p):
        return jnp.where(p < s, s - 1 - p, s), jnp.where(p < s, s, p - s)

    arrange(last)
    buf_a[...] = score(*last_pair(last, 0))

    def release(t, carry):
        q0, q1 = two_pairs(last_pair, last, t)
        finish(q0)

        @pl.when(t < 3)
        def _():
            finish(q1)

        return carry

    lax.fori_loop(0, 4, release, 0)

    def own_last(t, carry):
        two_pairs(last_pair, last, t)
        return carry

    lax.fori_loop(4, 7, own_last, 0)
    absorb(*last_pair(last, 2 * last), buf_a)
    finish(last)
    for item in loads[5:]:
        item.wait()

    def collect(s, carry):
        for piece in range(4):
            plane = y_low if piece < 2 else 1 - y_low
            from_z, _ = chunk_of(s, 1 - piece % 2)
            _, at_half = chunk_of(s, piece % 2)
            head = ((x + from_z % 4) % 4) * 4 + ((y_high + from_z // 4) % 2) * 2 + plane
            got = remote(
                out_stage.at[s, piece], att.at[head, at_half], out_send.at[s, piece],
                out_recv.at[s, piece], from_z * 2 + plane, grp,
            )
            if piece < 2:
                @pl.when(s > 0)
                def _():
                    got.wait_recv()
                    got.wait_send()
            else:
                got.wait_recv()
                got.wait_send()
        return carry

    lax.fori_loop(0, SETS, collect, 0)

    quarter = half // 2
    for side in range(2):
        for two in range(HEADS // 2):
            one = att[2 * two, side].astype(jnp.float32)
            other = att[2 * two + 1, side].astype(jnp.float32)
            top = jnp.where(lane < 64, one, pltpu.roll(other, 64, 1))
            low = jnp.where(lane < 64, pltpu.roll(one, 64, 1), other)
            span = slice(two * 128, (two + 1) * 128)
            at = side * half
            attended[at : at + quarter, span] = top.astype(jnp.bfloat16)
            attended[at + quarter : at + half, span] = low.astype(jnp.bfloat16)

    frames = jnp.concatenate([from_low[7], from_high[7]], axis=0).astype(jnp.float32)
    added = (
        frames + jnp.dot(attended[...], w_out[...], preferred_element_type=jnp.float32)
    ).astype(jnp.bfloat16)
    residual[...] = added
    conv_in = normalize(added.astype(jnp.float32), conv_gain[...]).astype(jnp.bfloat16)
    width = added.shape[1]
    columns = width // 128
    for column in range(0, width, 256):
        values = jnp.dot(
            conv_in, w_glu[:, column : column + 256], preferred_element_type=jnp.float32
        )
        gates = jnp.dot(
            conv_in, w_glu[:, width + column : width + column + 256],
            preferred_element_type=jnp.float32,
        )
        gated = (values * jax.nn.sigmoid(gates)).astype(jnp.bfloat16)
        edge_out[0, :, column : column + 256] = gated[:HALO]
        edge_out[1, :, column : column + 256] = gated[rows - HALO :]
        wide = gated.astype(jnp.float32)
        for c in range(2):
            tall[column // 128 + c, HALO : HALO + rows] = wide[:, c * 128 : (c + 1) * 128]

    to_left = remote(edge_out.at[0], edge_in.at[1], halo_send.at[0], halo_recv.at[0], *left)
    to_right = remote(edge_out.at[1], edge_in.at[0], halo_send.at[1], halo_recv.at[1], *right)
    to_left.start()
    to_right.start()

    taps = w_depth.shape[0]
    reach = taps // 2
    block = 64
    first_frame = (grp * 16 + blk) * rows

    def convolve(base):
        at = lax.broadcasted_iota(jnp.int32, (block, 128), 0) + (first_frame + base)
        first = jnp.zeros((block, 128), jnp.int32)
        final = jnp.zeros((block, 128), jnp.int32)
        begun = jnp.int32(0)
        for c in range(8):
            over = begun + utt[c]
            first = jnp.where(at >= begun, begun, first)
            final = jnp.where(at >= begun, over, final)
            begun = over
        first_tap = first - at + reach
        last_tap = final - at + reach
        for t in range(taps):
            valid[t] = jnp.where((first_tap <= t) & (last_tap > t), 1.0, 0.0)

        def column_of(c, carry):
            total = jnp.zeros((block, 128), jnp.float32)
            for t in range(taps):
                total = total + (
                    tall[c, pl.ds(base + (HALO - reach + t), block)] * valid[t]
                    * w_depth[t : t + 1, pl.ds(pl.multiple_of(c * 128, 128), 128)]
                )
            mixed[c] = total
            return carry

        lax.fori_loop(0, columns, column_of, 0)
        pieces = [mixed[c] for c in range(columns)]
        mean = jnp.sum(functools.reduce(jnp.add, pieces), axis=1, keepdims=True) / width
        pieces = [piece - mean for piece in pieces]
        spread = (
            jnp.sum(functools.reduce(jnp.add, [p * p for p in pieces]), axis=1, keepdims=True)
            / width
        )
        factor = lax.rsqrt(spread + epsilon)
        for c in range(columns):
            span = slice(c * 128, (c + 1) * 128)
            value = pieces[c] * factor * depth_gain[:, span]
            attended[pl.ds(base, block), span] = (value * jax.nn.sigmoid(value)).astype(
                jnp.bfloat16
            )

    def conv_step(index, carry):
        @pl.when(index == rows // block - 2)
        def _():
            to_left.wait_recv()
            to_right.wait_recv()
            for c in range(columns):
                span = slice(c * 128, (c + 1) * 128)
                tall[c, :HALO] = edge_in[0, :, span].astype(jnp.float32)
                tall[c, HALO + rows :] = edge_in[1, :, span].astype(jnp.float32)

        convolve(pl.multiple_of((index + 1) % (rows // block) * block, block))
        return carry

    lax.fori_loop(0, rows // block, conv_step, 0)
    for column in range(0, width, 256):
        span = slice(column, column + 256)
        out_ref[:, span] = (
            residual[:, span].astype(jnp.float32)
            + jnp.dot(attended[...], w_proj[:, span], preferred_element_type=jnp.float32)
        ).astype(jnp.bfloat16)

    for event in range(7):
        low_copy(event, from_low.at[event]).wait_send()
        high_copy(event, from_high.at[event]).wait_send()
    for s in range(SETS):
        for side in range(2):
            swap_copy(s, side).wait_send()
    core_copy.wait_send()

    @pl.when(z > 0)
    def _():
        w_copy.wait_send()

    to_left.wait_send()
    to_right.wait_send()


def block_of(
    frames, utt_lengths, attn_gain, w_qkv, w_out, conv_gain, w_glu, w_depth, depth_gain, w_proj
):
    rows, width = frames.shape
    half = rows // 2
    columns = width // 128
    taps = w_depth.shape[0]
    hbm = pl.BlockSpec(memory_space=pltpu.HBM)
    dma = pltpu.SemaphoreType.DMA
    bf16, f32 = jnp.bfloat16, jnp.float32
    return pl.pallas_call(
        mixing_kernel,
        out_shape=jax.ShapeDtypeStruct((rows, width), bf16),
        in_specs=[hbm] * 10,
        out_specs=pl.BlockSpec(memory_space=pltpu.VMEM),
        scratch_shapes=[
            pltpu.SMEM((8,), jnp.int32),
            pltpu.VMEM((1, width), f32),
            pltpu.VMEM((1, width), f32),
            pltpu.VMEM((1, width), f32),
            pltpu.VMEM((192, width), bf16),
            pltpu.VMEM((width, width), bf16),
            pltpu.VMEM((width, 2 * width), bf16),
            pltpu.VMEM((taps, width), f32),
            pltpu.VMEM((width, width), bf16),
            pltpu.VMEM((8, half, width), bf16),
            pltpu.VMEM((8, half, width), bf16),
            pltpu.VMEM((2, 192, width), bf16),
            pltpu.VMEM((SETS, 2, half, 256), bf16),
            pltpu.VMEM((SETS, 2 * rows, 256), bf16),
            pltpu.VMEM((SETS, 2 * rows, 128), bf16),
            pltpu.VMEM((SETS, 2 * rows, 128), bf16),
            pltpu.VMEM((SETS, 2 * rows, 128), f32),
            pltpu.VMEM((SETS, 2 * rows, 128), f32),
            pltpu.VMEM((2 * rows, 2 * rows), f32),
            pltpu.VMEM((2 * rows, 2 * rows), f32),
            pltpu.VMEM((SETS, 4, half // 2, 128), bf16),
            pltpu.VMEM((HEADS, 2, half // 2, 128), bf16),
            pltpu.VMEM((rows, width), bf16),
            pltpu.VMEM((rows, width), bf16),
            pltpu.VMEM((2, HALO, width), bf16),
            pltpu.VMEM((2, HALO, width), bf16),
            pltpu.VMEM((columns, rows + 2 * HALO, 128), f32),
            pltpu.VMEM((taps, 64, 128), f32),
            pltpu.VMEM((columns, 64, 128), f32),
            dma((11,)),
            dma((7,)), dma((7,)), dma((7,)), dma((7,)),
            dma, dma, dma, dma,
            dma((SETS, 2)), dma((SETS, 2)),
            dma((SETS, 4)), dma((SETS, 4)),
            dma((2,)), dma((2,)),
        ],
        compiler_params=pltpu.CompilerParams(
            collective_id=0, has_side_effects=True, vmem_limit_bytes=67043328
        ),
    )(
        utt_lengths, frames, attn_gain.reshape(1, width), w_qkv.T, w_out,
        conv_gain.reshape(1, width), w_glu, w_depth, depth_gain.reshape(1, width), w_proj,
    )


def body(frames, *others):
    return block_of(frames[0], *others)[None]


def solution(mesh):
    in_specs = (P("grp", "blk", None), P(), P(), P(None, "grp"), P(), P(), P(), P(), P(), P())
    out_specs = P("grp", "blk", None)
    return jax.shard_map(body, mesh=mesh, in_specs=in_specs, out_specs=out_specs, check_vma=False)
```

```python
import functools
import math

import jax
import jax.numpy as jnp
from jax import lax
from jax.experimental import pallas as pl
from jax.experimental.pallas import tpu as pltpu
from jax.sharding import PartitionSpec as P

SETS = 8
NEAR = 4
HALO = 16
MESH = pl.DeviceIdType.MESH

epsilon = 1e-05
big_negative = -1e30
lowest = -2e38


def normalize(values, row_gain):
    center = values - jnp.mean(values, axis=-1, keepdims=True)
    spread = jnp.mean(center * center, axis=-1, keepdims=True)
    return center * lax.rsqrt(spread + epsilon) * row_gain


def mixing_kernel(
    utt_hbm, frames_hbm, gain_hbm, w_hbm, w_out_hbm, conv_gain_hbm, w_glu_hbm, w_depth_hbm,
    depth_gain_hbm, w_proj_hbm,
    out_ref,
    utt, gain, conv_gain, depth_gain, w_mine, w_out, w_glu, w_depth, w_proj,
    from_low, from_high, w_kv, w_q, kv_stage, q_stage, kv_land, q_land, query, keys, vals,
    peak, mix, buf_a, buf_b, out_stage, attended, activated, residual, edge_out, edge_in, tall, valid, mixed,
    load_sem, low_send, low_recv, high_send, high_recv, w_send, w_recv, core_send, core_recv,
    kv_send, kv_recv, q_send, q_recv, out_send, out_recv, halo_send, halo_recv,
):
    half = from_low.shape[1]
    rows = 2 * half
    blk = lax.axis_index("blk")
    grp = lax.axis_index("grp")
    z, y_low = blk // 2, blk % 2
    x, y_high, core = grp // 4, (grp // 2) % 2, grp % 2
    quad = z % 4

    def member(of_quad, m):
        odd = of_quad % 2
        return jnp.where(odd == 1, of_quad, 2 * m), jnp.where(odd == 1, m, of_quad // 2)

    def head_of(of_quad, m, of_core):
        right_by, across = member(of_quad, m)
        return ((x + right_by) % 4) * 4 + ((y_high + across) % 2) * 2 + of_core

    other_core = grp + 1 - 2 * core
    partner = blk + 1 - 2 * y_low

    def w_from(m):
        return jnp.where(member(quad, m)[1] == 1, partner, blk), head_of(quad, m, core)

    def w_to(m):
        right_by, across = member(quad, m)
        return (
            jnp.where(across == 1, partner, blk),
            ((x + 4 - right_by) % 4) * 4 + ((y_high + across) % 2) * 2 + core,
        )

    def unless_own(m, act):
        if m == 1:
            act()
        else:
            pl.when(quad > 0)(act)
    z_up = (blk + 2) % 16
    z_down = (blk + 14) % 16
    left = ((blk + 15) % 16, (grp + jnp.where(blk == 0, 15, 0)) % 16)
    right = ((blk + 1) % 16, (grp + jnp.where(blk == 15, 1, 0)) % 16)

    def place(b, g):
        return {"blk": b, "grp": g}

    def load(index, src, dst):
        return pltpu.make_async_copy(src, dst, load_sem.at[index])

    loads = [
        load(0, frames_hbm.at[pl.ds(0, half)], from_low.at[7]),
        load(1, frames_hbm.at[pl.ds(half, half)], from_high.at[7]),
        load(2, w_hbm, w_mine),
        load(3, gain_hbm, gain),
        load(4, utt_hbm, utt),
        load(5, conv_gain_hbm, conv_gain),
        load(7, w_glu_hbm, w_glu),
        load(8, w_depth_hbm, w_depth),
        load(9, depth_gain_hbm, depth_gain),
        load(6, w_proj_hbm, w_proj),
    ]
    for slot in range(SETS):
        for m in range(2):
            head = head_of(slot // 2, m, slot % 2)
            loads.append(
                load(
                    10 + 2 * slot + m,
                    w_out_hbm.at[pl.ds(pl.multiple_of(head * 64, 64), 64)],
                    w_out.at[pl.ds(slot * 128 + m * 64, 64)],
                )
            )
    for item in loads:
        item.start()

    barrier = pltpu.get_barrier_semaphore()

    def greet(b, g):
        pl.semaphore_signal(barrier, inc=1, device_id=place(b, g), device_id_type=MESH)

    for step in range(1, 16):
        greet((blk + step) % 16, grp)
    greet(blk, other_core)
    greet(*left)
    greet(*right)

    for m in range(2):
        def greet_both(m=m):
            greet(*w_to(m))
            greet(*w_from(m))

        unless_own(m, greet_both)

    pl.semaphore_wait(barrier, jnp.where(quad > 0, 22, 20))

    def remote(src, dst, send, recv, b, g):
        return pltpu.make_async_remote_copy(
            src_ref=src, dst_ref=dst, send_sem=send, recv_sem=recv,
            device_id=place(b, g), device_id_type=MESH,
        )

    def low_copy(event, src):
        return remote(src, from_low.at[event], low_send.at[event], low_recv.at[event], z_up, grp)

    def high_copy(event, src):
        return remote(
            src, from_high.at[event], high_send.at[event], high_recv.at[event], z_down, grp
        )

    loads[0].wait()
    loads[1].wait()
    low_copy(0, from_low.at[7]).start()
    high_copy(0, from_high.at[7]).start()
    low_copy(1, from_high.at[7]).start()
    high_copy(1, from_low.at[7]).start()
    loads[2].wait()

    def w_copies(m):
        return (
            remote(
                w_mine.at[pl.ds(64, 128)], w_kv.at[core, pl.ds(m * 128, 128)],
                w_send.at[m, 0], w_recv.at[m, 0], *w_to(m),
            ),
            remote(
                w_mine.at[pl.ds(0, 64)], w_q.at[core, pl.ds(m * 64, 64)],
                w_send.at[m, 1], w_recv.at[m, 1], *w_to(m),
            ),
        )

    def start_w(m):
        for item in w_copies(m):
            item.start()

    for m in range(2):
        unless_own(m, functools.partial(start_w, m))

    @pl.when(quad == 0)
    def _():
        w_kv[core, :128] = w_mine[64:]
        w_q[core, :64] = w_mine[:64]

    loads[3].wait()
    loads[4].wait()

    def arrive(event):
        low_copy(event, from_low.at[event]).wait_recv()

        @pl.when(event <= 4)
        def _():
            low_copy(event + 2, from_low.at[event]).start()

        high_copy(event, from_high.at[event]).wait_recv()

        @pl.when(event <= 4)
        def _():
            high_copy(event + 2, from_high.at[event]).start()

    arrive(0)
    arrive(1)

    def await_w(m):
        for item in w_copies(m):
            item.wait_recv()

    for m in range(2):
        unless_own(m, functools.partial(await_w, m))

    def core_copies(which):
        return (
            remote(
                w_kv.at[which], w_kv.at[which], core_send.at[0], core_recv.at[0], blk, other_core
            ),
            remote(w_q.at[which], w_q.at[which], core_send.at[1], core_recv.at[1], blk, other_core),
        )

    for item in core_copies(core):
        item.start()
    for item in core_copies(1 - core):
        item.wait_recv()

    lane = lax.broadcasted_iota(jnp.int32, (1, 128), 1)
    begin = jnp.zeros((1, 128), jnp.int32)
    end = jnp.zeros((1, 128), jnp.int32)
    start = jnp.int32(0)
    for c in range(8):
        stop = start + utt[c]
        begin = jnp.where(lane == 64 + c, start, begin)
        end = jnp.where(lane == 64 + c, stop, end)
        start = stop
    scale = math.log2(math.e) / 8.0

    def chunk_of(s, side):
        event = s + 7
        odd = event % 2
        away = jnp.where(s == 0, 0, jnp.where(s == 7, 4, (s + 1) // 2))
        if side == 0:
            return (z + 8 - away) % 8, jnp.where(s == 0, 0, odd)
        return (z + away) % 8, jnp.where(s == 0, 1, 1 - odd)

    def kv_copy(s):
        return remote(
            kv_stage.at[s], kv_land.at[s, pl.ds(rows, rows)], kv_send.at[s], kv_recv.at[s],
            partner, grp,
        )

    def q_copy(s):
        return remote(
            q_stage.at[s], q_land.at[s, pl.ds(rows, rows)], q_send.at[s], q_recv.at[s],
            partner, grp,
        )

    def times(values, weights):
        return lax.dot_general(
            values, weights, (((1,), (1,)), ((), ())), preferred_element_type=jnp.float32
        )

    def project(s):
        slot = (s + 7) % 8
        frames = jnp.concatenate([from_low[slot], from_high[slot]], axis=0).astype(jnp.float32)
        normed = normalize(frames, gain[...]).astype(jnp.bfloat16)
        kv_stage[s] = times(normed, w_kv[1 - y_low]).astype(jnp.bfloat16)
        kv_copy(s).start()

        @pl.when(s < NEAR)
        def _():
            q_stage[s] = (times(normed, w_q[1 - y_low]) * scale).astype(jnp.bfloat16)
            q_copy(s).start()
            q_land[s, :rows] = (times(normed, w_q[y_low]) * scale).astype(jnp.bfloat16)

        kv_land[s, :rows] = times(normed, w_kv[y_low]).astype(jnp.bfloat16)

    def marks(s, piece):
        from_z, from_half = chunk_of(s, piece % 2)
        plane = y_low if piece < 2 else 1 - y_low
        first = grp * (16 * rows) + (from_z * 2 + plane) * rows + from_half * half
        position = lax.broadcasted_iota(jnp.int32, (half, 128), 0) + first
        return ((position >= begin) & (position < end)).astype(jnp.float32)

    def arrange(s):
        kv_copy(s).wait_recv()
        for piece in range(4):
            span = slice(piece * half, (piece + 1) * half)
            inside = marks(s, piece)
            for m in range(2):
                both = kv_land[s, span, m * 128 : (m + 1) * 128].astype(jnp.float32)
                keys[m, s, span] = jnp.where(lane < 64, both, inside).astype(jnp.bfloat16)
                vals[m, s, span] = jnp.where(lane < 64, 1.0, both).astype(jnp.bfloat16)

        @pl.when(s < NEAR)
        def _():
            q_copy(s).wait_recv()
            for piece in range(4):
                span = slice(piece * half, (piece + 1) * half)
                outside = jnp.where(lane < 72, (1.0 - marks(s, piece)) * big_negative, 0.0)
                both = q_land[s, span].astype(jnp.float32)
                query[0, s, span] = jnp.where(lane < 64, both, outside).astype(jnp.bfloat16)
                query[1, s, span] = jnp.where(lane < 64, pltpu.roll(both, 64, 1), outside).astype(
                    jnp.bfloat16
                )
            for m in range(2):
                peak[m, s] = jnp.full((2 * rows, 128), lowest, jnp.float32)
                mix[m, s] = jnp.zeros((2 * rows, 128), jnp.float32)

    def score(m, q, k):
        return times(query[m, q], keys[m, k])

    def absorb(m, q, k, buf):
        tiles = [buf[:, t * 128 : (t + 1) * 128] for t in range(2 * rows // 128)]
        old = peak[m, q]
        new = jnp.maximum(
            old, jnp.max(functools.reduce(jnp.maximum, tiles), axis=1, keepdims=True)
        )
        weights = jnp.concatenate(
            [jnp.exp2(tile - new).astype(jnp.bfloat16) for tile in tiles], axis=1
        )
        mix[m, q] = mix[m, q] * jnp.exp2(old - new) + jnp.dot(
            weights, vals[m, k], preferred_element_type=jnp.float32
        )
        peak[m, q] = new

    def pair(s, p):
        near = s < NEAR
        return (
            jnp.where(near, jnp.where(p <= s, s, p - s - 1), NEAR - 1 - p),
            jnp.where(near & (p <= s), p, s),
        )

    def both_heads(s, p):
        q, k = pair(s, p)
        buf_b[...] = score(1, q, k)
        absorb(0, q, k, buf_a)
        buf_a[...] = score(0, *pair(s, p + 1))
        absorb(1, q, k, buf_b)

    def last_heads(s, p):
        q, k = pair(s, p)
        buf_b[...] = score(1, q, k)
        absorb(0, q, k, buf_a)
        absorb(1, q, k, buf_b)

    def attend(s):
        count = jnp.where(s < NEAR, 2 * s + 1, NEAR)
        buf_a[...] = score(0, *pair(s, 0))

        def one(p, carry):
            both_heads(s, p)
            return carry

        lax.fori_loop(0, count - 1, one, 0)
        last_heads(s, count - 1)

    def step(s, carry):
        @pl.when(s >= 3)
        def _():
            arrive(s - 1)

        project(s)

        @pl.when(s >= 1)
        def _():
            arrange(s - 1)
            attend(s - 1)

        return carry

    lax.fori_loop(0, SETS, step, 0)

    slot_of_mine = quad * 2 + y_low

    def place_of(slot, at_half):
        return attended.at[
            pl.ds(pl.multiple_of(at_half * half, half), half),
            pl.ds(pl.multiple_of(slot * 128, 128), 128),
        ]

    def out_copy(s, piece):
        to_z, to_half = chunk_of(s, piece % 2)
        plane = y_low if piece < 2 else 1 - y_low
        return remote(
            out_stage.at[s, piece], place_of(slot_of_mine, to_half), out_send.at[s, piece],
            out_recv.at[s, piece], to_z * 2 + plane, grp,
        )

    def finish(s):
        one, other = (mix[m, s] / pltpu.roll(mix[m, s], 64, 1) for m in range(2))
        packed = jnp.where(lane < 64, pltpu.roll(one, 64, 1), other).astype(jnp.bfloat16)

        @pl.when(s > 0)
        def _():
            for piece in range(2):
                out_stage[s, piece] = packed[piece * half : (piece + 1) * half]
                out_copy(s, piece).start()

        @pl.when(s == 0)
        def _():
            mine = pl.ds(pl.multiple_of(slot_of_mine * 128, 128), 128)
            attended[:rows, mine] = packed[:rows]

        for piece in range(2, 4):
            out_stage[s, piece] = packed[piece * half : (piece + 1) * half]
            out_copy(s, piece).start()

    last = SETS - 1
    arrange(last)
    buf_a[...] = score(0, *pair(last, 0))

    def release(p, carry):
        both_heads(last, p)
        finish(pair(last, p)[0])
        return carry

    lax.fori_loop(0, NEAR - 1, release, 0)
    last_heads(last, NEAR - 1)
    finish(0)
    for item in loads[5:]:
        item.wait()

    def collect(s, carry):
        for piece in range(4):
            plane = y_low if piece < 2 else 1 - y_low
            from_z, _ = chunk_of(s, 1 - piece % 2)
            _, at_half = chunk_of(s, piece % 2)
            got = remote(
                out_stage.at[s, piece], place_of(from_z % 4 * 2 + plane, at_half),
                out_send.at[s, piece], out_recv.at[s, piece], from_z * 2 + plane, grp,
            )

            def settle(got=got):
                got.wait_recv()
                got.wait_send()

            if piece < 2:
                pl.when(s > 0)(settle)
            else:
                settle()
        return carry

    lax.fori_loop(0, NEAR, collect, 0)

    frames = jnp.concatenate([from_low[7], from_high[7]], axis=0).astype(jnp.float32)
    added = (
        frames + jnp.dot(attended[...], w_out[...], preferred_element_type=jnp.float32)
    ).astype(jnp.bfloat16)
    residual[...] = added
    conv_in = normalize(added.astype(jnp.float32), conv_gain[...]).astype(jnp.bfloat16)
    width = added.shape[1]
    columns = width // 128
    for column in range(0, width, 256):
        values = jnp.dot(
            conv_in, w_glu[:, column : column + 256], preferred_element_type=jnp.float32
        )
        gates = jnp.dot(
            conv_in, w_glu[:, width + column : width + column + 256],
            preferred_element_type=jnp.float32,
        )
        gated = (values * jax.nn.sigmoid(gates)).astype(jnp.bfloat16)
        edge_out[0, :, column : column + 256] = gated[:HALO]
        edge_out[1, :, column : column + 256] = gated[rows - HALO :]
        wide = gated.astype(jnp.float32)
        for c in range(2):
            tall[column // 128 + c, HALO : HALO + rows] = wide[:, c * 128 : (c + 1) * 128]

    to_left = remote(edge_out.at[0], edge_in.at[1], halo_send.at[0], halo_recv.at[0], *left)
    to_right = remote(edge_out.at[1], edge_in.at[0], halo_send.at[1], halo_recv.at[1], *right)
    to_left.start()
    to_right.start()

    taps = w_depth.shape[0]
    reach = taps // 2
    block = 64
    first_frame = (grp * 16 + blk) * rows

    def convolve(base):
        at = lax.broadcasted_iota(jnp.int32, (block, 128), 0) + (first_frame + base)
        first = jnp.zeros((block, 128), jnp.int32)
        final = jnp.zeros((block, 128), jnp.int32)
        begun = jnp.int32(0)
        for c in range(8):
            over = begun + utt[c]
            first = jnp.where(at >= begun, begun, first)
            final = jnp.where(at >= begun, over, final)
            begun = over
        first_tap = first - at + reach
        last_tap = final - at + reach
        for t in range(taps):
            valid[t] = jnp.where((first_tap <= t) & (last_tap > t), 1.0, 0.0)

        def column_of(c, carry):
            total = jnp.zeros((block, 128), jnp.float32)
            for t in range(taps):
                total = total + (
                    tall[c, pl.ds(base + (HALO - reach + t), block)] * valid[t]
                    * w_depth[t : t + 1, pl.ds(pl.multiple_of(c * 128, 128), 128)]
                )
            mixed[c] = total
            return carry

        lax.fori_loop(0, columns, column_of, 0)
        pieces = [mixed[c] for c in range(columns)]
        mean = jnp.sum(functools.reduce(jnp.add, pieces), axis=1, keepdims=True) / width
        pieces = [piece - mean for piece in pieces]
        spread = (
            jnp.sum(functools.reduce(jnp.add, [p * p for p in pieces]), axis=1, keepdims=True)
            / width
        )
        factor = lax.rsqrt(spread + epsilon)
        for c in range(columns):
            span = slice(c * 128, (c + 1) * 128)
            value = pieces[c] * factor * depth_gain[:, span]
            activated[pl.ds(base, block), span] = (value * jax.nn.sigmoid(value)).astype(
                jnp.bfloat16
            )

    def conv_step(index, carry):
        @pl.when(index == rows // block - 2)
        def _():
            to_left.wait_recv()
            to_right.wait_recv()
            for c in range(columns):
                span = slice(c * 128, (c + 1) * 128)
                tall[c, :HALO] = edge_in[0, :, span].astype(jnp.float32)
                tall[c, HALO + rows :] = edge_in[1, :, span].astype(jnp.float32)

        convolve(pl.multiple_of((index + 1) % (rows // block) * block, block))
        return carry

    lax.fori_loop(0, rows // block, conv_step, 0)
    for column in range(0, width, 256):
        span = slice(column, column + 256)
        out_ref[:, span] = (
            residual[:, span].astype(jnp.float32)
            + jnp.dot(activated[...], w_proj[:, span], preferred_element_type=jnp.float32)
        ).astype(jnp.bfloat16)

    for event in range(7):
        low_copy(event, from_low.at[event]).wait_send()
        high_copy(event, from_high.at[event]).wait_send()
    for s in range(SETS):
        kv_copy(s).wait_send()
    for s in range(NEAR):
        q_copy(s).wait_send()
    for item in core_copies(core):
        item.wait_send()

    def sent_w(m):
        for item in w_copies(m):
            item.wait_send()

    for m in range(2):
        unless_own(m, functools.partial(sent_w, m))
    to_left.wait_send()
    to_right.wait_send()


def block_of(
    frames, utt_lengths, attn_gain, w_qkv, w_out, conv_gain, w_glu, w_depth, depth_gain, w_proj
):
    rows, width = frames.shape
    half = rows // 2
    columns = width // 128
    taps = w_depth.shape[0]
    hbm = pl.BlockSpec(memory_space=pltpu.HBM)
    dma = pltpu.SemaphoreType.DMA
    bf16, f32 = jnp.bfloat16, jnp.float32
    return pl.pallas_call(
        mixing_kernel,
        out_shape=jax.ShapeDtypeStruct((rows, width), bf16),
        in_specs=[hbm] * 10,
        out_specs=pl.BlockSpec(memory_space=pltpu.VMEM),
        scratch_shapes=[
            pltpu.SMEM((8,), jnp.int32),
            pltpu.VMEM((1, width), f32),
            pltpu.VMEM((1, width), f32),
            pltpu.VMEM((1, width), f32),
            pltpu.VMEM((192, width), bf16),
            pltpu.VMEM((width, width), bf16),
            pltpu.VMEM((width, 2 * width), bf16),
            pltpu.VMEM((taps, width), f32),
            pltpu.VMEM((width, width), bf16),
            pltpu.VMEM((8, half, width), bf16),
            pltpu.VMEM((8, half, width), bf16),
            pltpu.VMEM((2, 256, width), bf16),
            pltpu.VMEM((2, 128, width), bf16),
            pltpu.VMEM((SETS, rows, 256), bf16),
            pltpu.VMEM((NEAR, rows, 128), bf16),
            pltpu.VMEM((SETS, 2 * rows, 256), bf16),
            pltpu.VMEM((NEAR, 2 * rows, 128), bf16),
            pltpu.VMEM((2, NEAR, 2 * rows, 128), bf16),
            pltpu.VMEM((2, SETS, 2 * rows, 128), bf16),
            pltpu.VMEM((2, SETS, 2 * rows, 128), bf16),
            pltpu.VMEM((2, NEAR, 2 * rows, 128), f32),
            pltpu.VMEM((2, NEAR, 2 * rows, 128), f32),
            pltpu.VMEM((2 * rows, 2 * rows), f32),
            pltpu.VMEM((2 * rows, 2 * rows), f32),
            pltpu.VMEM((NEAR, 4, half, 128), bf16),
            pltpu.VMEM((rows, width), bf16),
            pltpu.VMEM((rows, width), bf16),
            pltpu.VMEM((rows, width), bf16),
            pltpu.VMEM((2, HALO, width), bf16),
            pltpu.VMEM((2, HALO, width), bf16),
            pltpu.VMEM((columns, rows + 2 * HALO, 128), f32),
            pltpu.VMEM((taps, 64, 128), f32),
            pltpu.VMEM((columns, 64, 128), f32),
            dma((26,)),
            dma((7,)), dma((7,)), dma((7,)), dma((7,)),
            dma((2, 2)), dma((2, 2)), dma((2,)), dma((2,)),
            dma((SETS,)), dma((SETS,)), dma((NEAR,)), dma((NEAR,)),
            dma((NEAR, 4)), dma((NEAR, 4)),
            dma((2,)), dma((2,)),
        ],
        compiler_params=pltpu.CompilerParams(
            collective_id=0, has_side_effects=True, vmem_limit_bytes=67043328
        ),
    )(
        utt_lengths, frames, attn_gain.reshape(1, width), w_qkv.T, w_out,
        conv_gain.reshape(1, width), w_glu, w_depth, depth_gain.reshape(1, width), w_proj,
    )


def body(frames, *others):
    return block_of(frames[0], *others)[None]


def solution(mesh):
    in_specs = (P("grp", "blk", None), P(), P(), P(None, "grp"), P(), P(), P(), P(), P(), P())
    out_specs = P("grp", "blk", None)
    return jax.shard_map(body, mesh=mesh, in_specs=in_specs, out_specs=out_specs, check_vma=False)
```

```python
import functools
import math

import jax
import jax.numpy as jnp
from jax import lax
from jax.experimental import pallas as pl
from jax.experimental.pallas import tpu as pltpu
from jax.sharding import PartitionSpec as P

SETS = 8
NEAR = 4
HALO = 16
MESH = pl.DeviceIdType.MESH

epsilon = 1e-05
big_negative = -1e30
lowest = -2e38


def normalize(values, row_gain):
    center = values - jnp.mean(values, axis=-1, keepdims=True)
    spread = jnp.mean(center * center, axis=-1, keepdims=True)
    return center * lax.rsqrt(spread + epsilon) * row_gain


def mixing_kernel(
    utt_hbm, frames_hbm, gain_hbm, w_hbm, w_out_hbm, conv_gain_hbm, w_glu_hbm, w_depth_hbm,
    depth_gain_hbm, w_proj_hbm,
    out_ref,
    utt, gain, conv_gain, depth_gain, w_mine, w_out, w_glu, w_depth, w_proj,
    own, from_low, from_high, w_relay, w_kv, w_q, kv_stage, q_stage, kv_land, q_land, query, keys, vals,
    peak, mix, buf_a, buf_b, out_stage, attended, activated, residual, edge_out, edge_in, tall, valid, mixed,
    load_sem, low_send, low_recv, high_send, high_recv, w_send, w_recv, relay_send, relay_recv,
    far_send, core_send, core_recv,
    kv_send, kv_recv, q_send, q_recv, out_send, out_recv, halo_send, halo_recv,
):
    half = from_low.shape[1]
    rows = 2 * half
    blk = lax.axis_index("blk")
    grp = lax.axis_index("grp")
    z, y_low = blk // 2, blk % 2
    x, y_high, core = grp // 4, (grp // 2) % 2, grp % 2
    quad = z % 4

    def member(of_quad, m):
        return (of_quad + 2 * m) % 4, m

    def head_of(of_quad, m, of_core):
        right_by, across = member(of_quad, m)
        return ((x + right_by) % 4) * 4 + ((y_high + across) % 2) * 2 + of_core

    other_core = grp + 1 - 2 * core
    partner = blk + 1 - 2 * y_low

    def w_from(m):
        return jnp.where(member(quad, m)[1] == 1, partner, blk), head_of(quad, m, core)

    def w_to(m):
        right_by, across = member(quad, m)
        return (
            jnp.where(across == 1, partner, blk),
            ((x + 4 - right_by) % 4) * 4 + ((y_high + across) % 2) * 2 + core,
        )

    even = quad % 2 == 0
    far = jnp.where(quad == 0, 1, 0)
    stride = jnp.where(core == 0, 3, 1)

    def along(count, across):
        return (
            jnp.where(across == 1, partner, blk),
            ((x + count) % 4) * 4 + ((y_high + across) % 2) * 2 + core,
        )

    relay_to, relay_from = along(stride, 0), along(4 - stride, 0)
    far_to, far_from = along(stride, far), along(4 - stride, far)

    def if_direct(m, act):
        pl.when(quad > 0 if m == 1 else quad % 2 == 1)(act)

    def if_sent(m, act):
        if m == 1:
            act()
        else:
            pl.when(quad > 0)(act)

    z_up = (blk + 2) % 16
    z_down = (blk + 14) % 16
    left = ((blk + 15) % 16, (grp + jnp.where(blk == 0, 15, 0)) % 16)
    right = ((blk + 1) % 16, (grp + jnp.where(blk == 15, 1, 0)) % 16)

    def place(b, g):
        return {"blk": b, "grp": g}

    def load(index, src, dst):
        return pltpu.make_async_copy(src, dst, load_sem.at[index])

    loads = [
        load(0, frames_hbm, own),
        load(1, conv_gain_hbm, conv_gain),
        load(2, w_hbm, w_mine),
        load(3, gain_hbm, gain),
        load(4, utt_hbm, utt),
        load(7, w_glu_hbm, w_glu),
        load(8, w_depth_hbm, w_depth),
        load(9, depth_gain_hbm, depth_gain),
        load(6, w_proj_hbm, w_proj),
    ]
    for slot in range(SETS):
        for m in range(2):
            head = head_of(slot // 2, m, slot % 2)
            loads.append(
                load(
                    10 + 2 * slot + m,
                    w_out_hbm.at[pl.ds(pl.multiple_of(head * 64, 64), 64)],
                    w_out.at[pl.ds(slot * 128 + m * 64, 64)],
                )
            )
    for item in loads:
        item.start()

    barrier = pltpu.get_barrier_semaphore()

    def greet(b, g):
        pl.semaphore_signal(barrier, inc=1, device_id=place(b, g), device_id_type=MESH)

    for step in range(1, 16):
        greet((blk + step) % 16, grp)
    greet(blk, other_core)
    greet(*left)
    greet(*right)

    for m in range(2):
        def greet_both(m=m):
            greet(*w_to(m))
            greet(*w_from(m))

        if_direct(m, greet_both)

    @pl.when(even)
    def _():
        for each in (relay_to, relay_from, far_to, far_from):
            greet(*each)

    loads[0].wait()
    loads[3].wait()
    for side, kept in ((0, from_low), (1, from_high)):
        kept[7] = normalize(
            own[side * half : (side + 1) * half].astype(jnp.float32), gain[...]
        ).astype(jnp.bfloat16)
    loads[2].wait()
    pl.semaphore_wait(barrier, jnp.where(quad == 2, 24, 22))

    def remote(src, dst, send, recv, b, g):
        return pltpu.make_async_remote_copy(
            src_ref=src, dst_ref=dst, send_sem=send, recv_sem=recv,
            device_id=place(b, g), device_id_type=MESH,
        )

    def low_copy(event, src):
        return remote(src, from_low.at[event], low_send.at[event], low_recv.at[event], z_up, grp)

    def high_copy(event, src):
        return remote(
            src, from_high.at[event], high_send.at[event], high_recv.at[event], z_down, grp
        )

    low_copy(0, from_low.at[7]).start()
    high_copy(0, from_high.at[7]).start()
    low_copy(1, from_high.at[7]).start()
    high_copy(1, from_low.at[7]).start()

    def w_copies(m):
        return (
            remote(
                w_mine.at[pl.ds(64, 128)], w_kv.at[core, pl.ds(m * 128, 128)],
                w_send.at[m, 0], w_recv.at[m, 0], *w_to(m),
            ),
            remote(
                w_mine.at[pl.ds(0, 64)], w_q.at[core, pl.ds(m * 64, 64)],
                w_send.at[m, 1], w_recv.at[m, 1], *w_to(m),
            ),
        )

    def start_w(m):
        for item in w_copies(m):
            item.start()

    def relay_copies():
        return [
            remote(
                w_mine.at[at], w_relay.at[at], relay_send.at[part], relay_recv.at[part], *relay_to
            )
            for part, at in enumerate((pl.ds(64, 128), pl.ds(0, 64)))
        ]

    def far_copies():
        return (
            remote(
                w_relay.at[pl.ds(64, 128)],
                w_kv.at[core, pl.ds(pl.multiple_of(far * 128, 128), 128)],
                far_send.at[0], w_recv.at[far, 0], *far_to,
            ),
            remote(
                w_relay.at[pl.ds(0, 64)],
                w_q.at[core, pl.ds(pl.multiple_of(far * 64, 64), 64)],
                far_send.at[1], w_recv.at[far, 1], *far_to,
            ),
        )

    @pl.when(even)
    def _():
        for item in relay_copies():
            item.start()

    for m in range(2):
        if_direct(m, functools.partial(start_w, m))

    @pl.when(quad == 0)
    def _():
        w_kv[core, :128] = w_mine[64:]
        w_q[core, :64] = w_mine[:64]

    @pl.when(even)
    def _():
        for came, item in zip(relay_copies(), far_copies()):
            came.wait_recv()
            item.start()

    loads[4].wait()

    def arrive(event):
        low_copy(event, from_low.at[event]).wait_recv()

        @pl.when(event <= 4)
        def _():
            low_copy(event + 2, from_low.at[event]).start()

        high_copy(event, from_high.at[event]).wait_recv()

        @pl.when(event <= 4)
        def _():
            high_copy(event + 2, from_high.at[event]).start()

    arrive(0)

    def await_w(m):
        for item in w_copies(m):
            item.wait_recv()

    for m in range(2):
        if_sent(m, functools.partial(await_w, m))

    def core_copies(which):
        return (
            remote(
                w_kv.at[which], w_kv.at[which], core_send.at[0], core_recv.at[0], blk, other_core
            ),
            remote(w_q.at[which], w_q.at[which], core_send.at[1], core_recv.at[1], blk, other_core),
        )

    for item in core_copies(core):
        item.start()
    for item in core_copies(1 - core):
        item.wait_recv()

    lane = lax.broadcasted_iota(jnp.int32, (1, 128), 1)
    begin = jnp.zeros((1, 128), jnp.int32)
    end = jnp.zeros((1, 128), jnp.int32)
    start = jnp.int32(0)
    for c in range(8):
        stop = start + utt[c]
        begin = jnp.where(lane == 64 + c, start, begin)
        end = jnp.where(lane == 64 + c, stop, end)
        start = stop
    scale = math.log2(math.e) / 8.0

    def chunk_of(s, side):
        event = s + 7
        odd = event % 2
        away = jnp.where(s == 0, 0, jnp.where(s == 7, 4, (s + 1) // 2))
        if side == 0:
            return (z + 8 - away) % 8, jnp.where(s == 0, 0, odd)
        return (z + away) % 8, jnp.where(s == 0, 1, 1 - odd)

    def kv_copy(s):
        return remote(
            kv_stage.at[s], kv_land.at[s, pl.ds(rows, rows)], kv_send.at[s], kv_recv.at[s],
            partner, grp,
        )

    def q_copy(s):
        return remote(
            q_stage.at[s], q_land.at[s, pl.ds(rows, rows)], q_send.at[s], q_recv.at[s],
            partner, grp,
        )

    def times(values, weights):
        return lax.dot_general(
            values, weights, (((1,), (1,)), ((), ())), preferred_element_type=jnp.float32
        )

    def project(s):
        slot = (s + 7) % 8
        normed = jnp.concatenate([from_low[slot], from_high[slot]], axis=0)
        kv_stage[s] = times(normed, w_kv[1 - y_low]).astype(jnp.bfloat16)
        kv_copy(s).start()

        @pl.when(s < NEAR)
        def _():
            q_stage[s] = (times(normed, w_q[1 - y_low]) * scale).astype(jnp.bfloat16)
            q_copy(s).start()
            q_land[s, :rows] = (times(normed, w_q[y_low]) * scale).astype(jnp.bfloat16)

        kv_land[s, :rows] = times(normed, w_kv[y_low]).astype(jnp.bfloat16)

    def marks(s, piece):
        from_z, from_half = chunk_of(s, piece % 2)
        plane = y_low if piece < 2 else 1 - y_low
        first = grp * (16 * rows) + (from_z * 2 + plane) * rows + from_half * half
        position = lax.broadcasted_iota(jnp.int32, (half, 128), 0) + first
        return ((position >= begin) & (position < end)).astype(jnp.float32)

    def arrange(s):
        kv_copy(s).wait_recv()
        for piece in range(4):
            span = slice(piece * half, (piece + 1) * half)
            inside = marks(s, piece)
            for m in range(2):
                both = kv_land[s, span, m * 128 : (m + 1) * 128].astype(jnp.float32)
                keys[m, s, span] = jnp.where(lane < 64, both, inside).astype(jnp.bfloat16)
                vals[m, s, span] = jnp.where(lane < 64, 1.0, both).astype(jnp.bfloat16)

        @pl.when(s < NEAR)
        def _():
            q_copy(s).wait_recv()
            for piece in range(4):
                span = slice(piece * half, (piece + 1) * half)
                outside = jnp.where(lane < 72, (1.0 - marks(s, piece)) * big_negative, 0.0)
                both = q_land[s, span].astype(jnp.float32)
                query[0, s, span] = jnp.where(lane < 64, both, outside).astype(jnp.bfloat16)
                query[1, s, span] = jnp.where(lane < 64, pltpu.roll(both, 64, 1), outside).astype(
                    jnp.bfloat16
                )
            for m in range(2):
                peak[m, s] = jnp.full((2 * rows, 128), lowest, jnp.float32)
                mix[m, s] = jnp.zeros((2 * rows, 128), jnp.float32)

    def score(m, q, k):
        return times(query[m, q], keys[m, k])

    def absorb(m, q, k, buf):
        tiles = [buf[:, t * 128 : (t + 1) * 128] for t in range(2 * rows // 128)]
        old = peak[m, q]
        new = jnp.maximum(
            old, jnp.max(functools.reduce(jnp.maximum, tiles), axis=1, keepdims=True)
        )
        weights = jnp.concatenate(
            [jnp.exp2(tile - new).astype(jnp.bfloat16) for tile in tiles], axis=1
        )
        mix[m, q] = mix[m, q] * jnp.exp2(old - new) + jnp.dot(
            weights, vals[m, k], preferred_element_type=jnp.float32
        )
        peak[m, q] = new

    def pair(s, p):
        near = s < NEAR
        return (
            jnp.where(near, jnp.where(p <= s, s, p - s - 1), NEAR - 1 - p),
            jnp.where(near & (p <= s), p, s),
        )

    def both_heads(s, p):
        q, k = pair(s, p)
        buf_b[...] = score(1, q, k)
        absorb(0, q, k, buf_a)
        buf_a[...] = score(0, *pair(s, p + 1))
        absorb(1, q, k, buf_b)

    def last_heads(s, p):
        q, k = pair(s, p)
        buf_b[...] = score(1, q, k)
        absorb(0, q, k, buf_a)
        absorb(1, q, k, buf_b)

    def attend(s):
        count = jnp.where(s < NEAR, 2 * s + 1, NEAR)
        buf_a[...] = score(0, *pair(s, 0))

        def one(p, carry):
            both_heads(s, p)
            return carry

        lax.fori_loop(0, count - 1, one, 0)
        last_heads(s, count - 1)

    def step(s, carry):
        @pl.when((s >= 2) & (s < SETS))
        def _():
            arrive(s - 1)

        @pl.when(s < SETS)
        def _():
            project(s)

        @pl.when(s >= 2)
        def _():
            arrange(s - 2)
            attend(s - 2)

        return carry

    lax.fori_loop(0, SETS + 1, step, 0)

    slot_of_mine = quad * 2 + y_low

    def place_of(slot, at_half):
        return attended.at[
            pl.ds(pl.multiple_of(at_half * half, half), half),
            pl.ds(pl.multiple_of(slot * 128, 128), 128),
        ]

    def out_copy(s, piece):
        to_z, to_half = chunk_of(s, piece % 2)
        plane = y_low if piece < 2 else 1 - y_low
        return remote(
            out_stage.at[s, piece], place_of(slot_of_mine, to_half), out_send.at[s, piece],
            out_recv.at[s, piece], to_z * 2 + plane, grp,
        )

    def finish(s):
        one, other = (mix[m, s] / pltpu.roll(mix[m, s], 64, 1) for m in range(2))
        packed = jnp.where(lane < 64, pltpu.roll(one, 64, 1), other).astype(jnp.bfloat16)

        @pl.when(s > 0)
        def _():
            for piece in range(2):
                out_stage[s, piece] = packed[piece * half : (piece + 1) * half]
                out_copy(s, piece).start()

        @pl.when(s == 0)
        def _():
            mine = pl.ds(pl.multiple_of(slot_of_mine * 128, 128), 128)
            attended[:rows, mine] = packed[:rows]

        for piece in range(2, 4):
            out_stage[s, piece] = packed[piece * half : (piece + 1) * half]
            out_copy(s, piece).start()

    last = SETS - 1
    arrange(last)
    buf_a[...] = score(0, *pair(last, 0))

    def release(p, carry):
        both_heads(last, p)
        finish(pair(last, p)[0])
        return carry

    lax.fori_loop(0, NEAR - 1, release, 0)
    last_heads(last, NEAR - 1)
    finish(0)
    for item in loads[1:2] + loads[5:]:
        item.wait()

    def collect(s, carry):
        for piece in range(4):
            plane = y_low if piece < 2 else 1 - y_low
            from_z, _ = chunk_of(s, 1 - piece % 2)
            _, at_half = chunk_of(s, piece % 2)
            got = remote(
                out_stage.at[s, piece], place_of(from_z % 4 * 2 + plane, at_half),
                out_send.at[s, piece], out_recv.at[s, piece], from_z * 2 + plane, grp,
            )

            def settle(got=got):
                got.wait_recv()
                got.wait_send()

            if piece < 2:
                pl.when(s > 0)(settle)
            else:
                settle()
        return carry

    lax.fori_loop(0, NEAR, collect, 0)

    added = (
        own[...].astype(jnp.float32) + jnp.dot(attended[...], w_out[...], preferred_element_type=jnp.float32)
    ).astype(jnp.bfloat16)
    residual[...] = added
    conv_in = normalize(added.astype(jnp.float32), conv_gain[...]).astype(jnp.bfloat16)
    width = added.shape[1]
    columns = width // 128
    for column in range(0, width, 256):
        values = jnp.dot(
            conv_in, w_glu[:, column : column + 256], preferred_element_type=jnp.float32
        )
        gates = jnp.dot(
            conv_in, w_glu[:, width + column : width + column + 256],
            preferred_element_type=jnp.float32,
        )
        gated = (values * jax.nn.sigmoid(gates)).astype(jnp.bfloat16)
        edge_out[0, :, column : column + 256] = gated[:HALO]
        edge_out[1, :, column : column + 256] = gated[rows - HALO :]
        wide = gated.astype(jnp.float32)
        for c in range(2):
            tall[column // 128 + c, HALO : HALO + rows] = wide[:, c * 128 : (c + 1) * 128]

    to_left = remote(edge_out.at[0], edge_in.at[1], halo_send.at[0], halo_recv.at[0], *left)
    to_right = remote(edge_out.at[1], edge_in.at[0], halo_send.at[1], halo_recv.at[1], *right)
    to_left.start()
    to_right.start()

    taps = w_depth.shape[0]
    reach = taps // 2
    block = 64
    first_frame = (grp * 16 + blk) * rows

    def convolve(base):
        at = lax.broadcasted_iota(jnp.int32, (block, 128), 0) + (first_frame + base)
        first = jnp.zeros((block, 128), jnp.int32)
        final = jnp.zeros((block, 128), jnp.int32)
        begun = jnp.int32(0)
        for c in range(8):
            over = begun + utt[c]
            first = jnp.where(at >= begun, begun, first)
            final = jnp.where(at >= begun, over, final)
            begun = over
        first_tap = first - at + reach
        last_tap = final - at + reach
        for t in range(taps):
            valid[t] = jnp.where((first_tap <= t) & (last_tap > t), 1.0, 0.0)

        def column_of(c, carry):
            total = jnp.zeros((block, 128), jnp.float32)
            for t in range(taps):
                total = total + (
                    tall[c, pl.ds(base + (HALO - reach + t), block)] * valid[t]
                    * w_depth[t : t + 1, pl.ds(pl.multiple_of(c * 128, 128), 128)]
                )
            mixed[c] = total
            return carry

        lax.fori_loop(0, columns, column_of, 0)
        pieces = [mixed[c] for c in range(columns)]
        mean = jnp.sum(functools.reduce(jnp.add, pieces), axis=1, keepdims=True) / width
        pieces = [piece - mean for piece in pieces]
        spread = (
            jnp.sum(functools.reduce(jnp.add, [p * p for p in pieces]), axis=1, keepdims=True)
            / width
        )
        factor = lax.rsqrt(spread + epsilon)
        for c in range(columns):
            span = slice(c * 128, (c + 1) * 128)
            value = pieces[c] * factor * depth_gain[:, span]
            activated[pl.ds(base, block), span] = (value * jax.nn.sigmoid(value)).astype(
                jnp.bfloat16
            )

    def conv_step(index, carry):
        @pl.when(index == rows // block - 2)
        def _():
            to_left.wait_recv()
            to_right.wait_recv()
            for c in range(columns):
                span = slice(c * 128, (c + 1) * 128)
                tall[c, :HALO] = edge_in[0, :, span].astype(jnp.float32)
                tall[c, HALO + rows :] = edge_in[1, :, span].astype(jnp.float32)

        convolve(pl.multiple_of((index + 1) % (rows // block) * block, block))
        return carry

    lax.fori_loop(0, rows // block, conv_step, 0)
    for column in range(0, width, 256):
        span = slice(column, column + 256)
        out_ref[:, span] = (
            residual[:, span].astype(jnp.float32)
            + jnp.dot(activated[...], w_proj[:, span], preferred_element_type=jnp.float32)
        ).astype(jnp.bfloat16)

    for event in range(7):
        low_copy(event, from_low.at[event]).wait_send()
        high_copy(event, from_high.at[event]).wait_send()
    for s in range(SETS):
        kv_copy(s).wait_send()
    for s in range(NEAR):
        q_copy(s).wait_send()
    for item in core_copies(core):
        item.wait_send()

    def sent_w(m):
        for item in w_copies(m):
            item.wait_send()

    for m in range(2):
        if_direct(m, functools.partial(sent_w, m))

    @pl.when(even)
    def _():
        for item in (*relay_copies(), *far_copies()):
            item.wait_send()

    to_left.wait_send()
    to_right.wait_send()


def block_of(
    frames, utt_lengths, attn_gain, w_qkv, w_out, conv_gain, w_glu, w_depth, depth_gain, w_proj
):
    rows, width = frames.shape
    half = rows // 2
    columns = width // 128
    taps = w_depth.shape[0]
    hbm = pl.BlockSpec(memory_space=pltpu.HBM)
    dma = pltpu.SemaphoreType.DMA
    bf16, f32 = jnp.bfloat16, jnp.float32
    return pl.pallas_call(
        mixing_kernel,
        out_shape=jax.ShapeDtypeStruct((rows, width), bf16),
        in_specs=[hbm] * 10,
        out_specs=pl.BlockSpec(memory_space=pltpu.VMEM),
        scratch_shapes=[
            pltpu.SMEM((8,), jnp.int32),
            pltpu.VMEM((1, width), f32),
            pltpu.VMEM((1, width), f32),
            pltpu.VMEM((1, width), f32),
            pltpu.VMEM((192, width), bf16),
            pltpu.VMEM((width, width), bf16),
            pltpu.VMEM((width, 2 * width), bf16),
            pltpu.VMEM((taps, width), f32),
            pltpu.VMEM((width, width), bf16),
            pltpu.VMEM((rows, width), bf16),
            pltpu.VMEM((8, half, width), bf16),
            pltpu.VMEM((8, half, width), bf16),
            pltpu.VMEM((192, width), bf16),
            pltpu.VMEM((2, 256, width), bf16),
            pltpu.VMEM((2, 128, width), bf16),
            pltpu.VMEM((SETS, rows, 256), bf16),
            pltpu.VMEM((NEAR, rows, 128), bf16),
            pltpu.VMEM((SETS, 2 * rows, 256), bf16),
            pltpu.VMEM((NEAR, 2 * rows, 128), bf16),
            pltpu.VMEM((2, NEAR, 2 * rows, 128), bf16),
            pltpu.VMEM((2, SETS, 2 * rows, 128), bf16),
            pltpu.VMEM((2, SETS, 2 * rows, 128), bf16),
            pltpu.VMEM((2, NEAR, 2 * rows, 128), f32),
            pltpu.VMEM((2, NEAR, 2 * rows, 128), f32),
            pltpu.VMEM((2 * rows, 2 * rows), f32),
            pltpu.VMEM((2 * rows, 2 * rows), f32),
            pltpu.VMEM((NEAR, 4, half, 128), bf16),
            pltpu.VMEM((rows, width), bf16),
            pltpu.VMEM((rows, width), bf16),
            pltpu.VMEM((rows, width), bf16),
            pltpu.VMEM((2, HALO, width), bf16),
            pltpu.VMEM((2, HALO, width), bf16),
            pltpu.VMEM((columns, rows + 2 * HALO, 128), f32),
            pltpu.VMEM((taps, 64, 128), f32),
            pltpu.VMEM((columns, 64, 128), f32),
            dma((26,)),
            dma((7,)), dma((7,)), dma((7,)), dma((7,)),
            dma((2, 2)), dma((2, 2)), dma((2,)), dma((2,)), dma((2,)), dma((2,)), dma((2,)),
            dma((SETS,)), dma((SETS,)), dma((NEAR,)), dma((NEAR,)),
            dma((NEAR, 4)), dma((NEAR, 4)),
            dma((2,)), dma((2,)),
        ],
        compiler_params=pltpu.CompilerParams(
            collective_id=0, has_side_effects=True, vmem_limit_bytes=67043328
        ),
    )(
        utt_lengths, frames, attn_gain.reshape(1, width), w_qkv.T, w_out,
        conv_gain.reshape(1, width), w_glu, w_depth, depth_gain.reshape(1, width), w_proj,
    )


def body(frames, *others):
    return block_of(frames[0], *others)[None]


def solution(mesh):
    in_specs = (P("grp", "blk", None), P(), P(), P(None, "grp"), P(), P(), P(), P(), P(), P())
    out_specs = P("grp", "blk", None)
    return jax.shard_map(body, mesh=mesh, in_specs=in_specs, out_specs=out_specs, check_vma=False)
```

```python
import functools
import math

import jax
import jax.numpy as jnp
from jax import lax
from jax.experimental import pallas as pl
from jax.experimental.pallas import tpu as pltpu
from jax.sharding import PartitionSpec as P

SETS = 8
NEAR = 4
HALO = 16
MESH = pl.DeviceIdType.MESH

epsilon = 1e-05
big_negative = -1e30
lowest = -2e38


def normalize(values, row_gain):
    center = values - jnp.mean(values, axis=-1, keepdims=True)
    spread = jnp.mean(center * center, axis=-1, keepdims=True)
    return center * lax.rsqrt(spread + epsilon) * row_gain


def mixing_kernel(
    utt_hbm, frames_hbm, gain_hbm, w_hbm, w_out_hbm, conv_gain_hbm, w_glu_hbm, w_depth_hbm,
    depth_gain_hbm, w_proj_hbm,
    out_ref,
    utt, gain, conv_gain, depth_gain, w_mine, w_out, w_glu, w_depth, w_proj,
    own, from_low, from_high, w_relay, w_kv, w_q, kv_stage, q_stage, kv_land, q_land, query, keys, vals,
    peak, mix, buf_a, buf_b, out_stage, attended, activated, residual, edge_out, edge_in, tall, valid, mixed,
    load_sem, low_send, low_recv, high_send, high_recv, w_send, w_recv, relay_send, relay_recv,
    far_send, core_send, core_recv,
    kv_send, kv_recv, q_send, q_recv, out_send, out_recv, halo_send, halo_recv,
):
    half = from_low.shape[1]
    rows = 2 * half
    blk = lax.axis_index("blk")
    grp = lax.axis_index("grp")
    z, y_low = blk // 2, blk % 2
    x, y_high, core = grp // 4, (grp // 2) % 2, grp % 2
    quad = z % 4

    def member(of_quad, m):
        return (of_quad + 2 * m) % 4, m

    def head_of(of_quad, m, of_core):
        right_by, across = member(of_quad, m)
        return ((x + right_by) % 4) * 4 + ((y_high + across) % 2) * 2 + of_core

    other_core = grp + 1 - 2 * core
    partner = blk + 1 - 2 * y_low

    def w_from(m):
        return jnp.where(member(quad, m)[1] == 1, partner, blk), head_of(quad, m, core)

    def w_to(m):
        right_by, across = member(quad, m)
        return (
            jnp.where(across == 1, partner, blk),
            ((x + 4 - right_by) % 4) * 4 + ((y_high + across) % 2) * 2 + core,
        )

    even = quad % 2 == 0
    far = jnp.where(quad == 0, 1, 0)
    stride = jnp.where(core == 0, 3, 1)

    def along(count, across):
        return (
            jnp.where(across == 1, partner, blk),
            ((x + count) % 4) * 4 + ((y_high + across) % 2) * 2 + core,
        )

    relay_to, relay_from = along(stride, 0), along(4 - stride, 0)
    far_to, far_from = along(stride, far), along(4 - stride, far)

    def if_direct(m, act):
        pl.when(quad > 0 if m == 1 else quad % 2 == 1)(act)

    def if_sent(m, act):
        if m == 1:
            act()
        else:
            pl.when(quad > 0)(act)

    z_up = (blk + 2) % 16
    z_down = (blk + 14) % 16
    left = ((blk + 15) % 16, (grp + jnp.where(blk == 0, 15, 0)) % 16)
    right = ((blk + 1) % 16, (grp + jnp.where(blk == 15, 1, 0)) % 16)

    def place(b, g):
        return {"blk": b, "grp": g}

    def load(index, src, dst):
        return pltpu.make_async_copy(src, dst, load_sem.at[index])

    loads = [
        load(0, frames_hbm, own),
        load(1, conv_gain_hbm, conv_gain),
        load(2, w_hbm, w_mine),
        load(3, gain_hbm, gain),
        load(4, utt_hbm, utt),
        load(7, w_glu_hbm, w_glu),
        load(8, w_depth_hbm, w_depth),
        load(9, depth_gain_hbm, depth_gain),
        load(6, w_proj_hbm, w_proj),
    ]
    for slot in range(SETS):
        for m in range(2):
            head = head_of(slot // 2, m, slot % 2)
            loads.append(
                load(
                    10 + 2 * slot + m,
                    w_out_hbm.at[pl.ds(pl.multiple_of(head * 64, 64), 64)],
                    w_out.at[pl.ds(slot * 128 + m * 64, 64)],
                )
            )
    for item in loads:
        item.start()

    barrier = pltpu.get_barrier_semaphore()

    def greet(b, g):
        pl.semaphore_signal(barrier, inc=1, device_id=place(b, g), device_id_type=MESH)

    for step in range(1, 16):
        greet((blk + step) % 16, grp)
    greet(blk, other_core)
    greet(*left)
    greet(*right)

    for m in range(2):
        def greet_both(m=m):
            greet(*w_to(m))
            greet(*w_from(m))

        if_direct(m, greet_both)

    @pl.when(even)
    def _():
        for each in (relay_to, relay_from, far_to, far_from):
            greet(*each)

    loads[0].wait()
    loads[3].wait()
    for side, kept in ((0, from_low), (1, from_high)):
        kept[7] = normalize(
            own[side * half : (side + 1) * half].astype(jnp.float32), gain[...]
        ).astype(jnp.bfloat16)
    loads[2].wait()
    pl.semaphore_wait(barrier, jnp.where(quad == 2, 24, 22))

    def remote(src, dst, send, recv, b, g):
        return pltpu.make_async_remote_copy(
            src_ref=src, dst_ref=dst, send_sem=send, recv_sem=recv,
            device_id=place(b, g), device_id_type=MESH,
        )

    def low_copy(event, src):
        return remote(src, from_low.at[event], low_send.at[event], low_recv.at[event], z_up, grp)

    def high_copy(event, src):
        return remote(
            src, from_high.at[event], high_send.at[event], high_recv.at[event], z_down, grp
        )

    low_copy(0, from_low.at[7]).start()
    high_copy(0, from_high.at[7]).start()
    low_copy(1, from_high.at[7]).start()
    high_copy(1, from_low.at[7]).start()

    def w_copies(m):
        return (
            remote(
                w_mine.at[pl.ds(64, 128)], w_kv.at[core, pl.ds(m * 128, 128)],
                w_send.at[m, 0], w_recv.at[m, 0], *w_to(m),
            ),
            remote(
                w_mine.at[pl.ds(0, 64)], w_q.at[core, pl.ds(m * 64, 64)],
                w_send.at[m, 1], w_recv.at[m, 1], *w_to(m),
            ),
        )

    def start_w(m):
        for item in w_copies(m):
            item.start()

    def relay_copies():
        return [
            remote(
                w_mine.at[at], w_relay.at[at], relay_send.at[part], relay_recv.at[part], *relay_to
            )
            for part, at in enumerate((pl.ds(64, 128), pl.ds(0, 64)))
        ]

    def far_copies():
        return (
            remote(
                w_relay.at[pl.ds(64, 128)],
                w_kv.at[core, pl.ds(pl.multiple_of(far * 128, 128), 128)],
                far_send.at[0], w_recv.at[far, 0], *far_to,
            ),
            remote(
                w_relay.at[pl.ds(0, 64)],
                w_q.at[core, pl.ds(pl.multiple_of(far * 64, 64), 64)],
                far_send.at[1], w_recv.at[far, 1], *far_to,
            ),
        )

    @pl.when(even)
    def _():
        for item in relay_copies():
            item.start()

    for m in range(2):
        if_direct(m, functools.partial(start_w, m))

    @pl.when(quad == 0)
    def _():
        w_kv[core, :128] = w_mine[64:]
        w_q[core, :64] = w_mine[:64]

    @pl.when(even)
    def _():
        for came, item in zip(relay_copies(), far_copies()):
            came.wait_recv()
            item.start()

    loads[4].wait()

    def arrive(event):
        low_copy(event, from_low.at[event]).wait_recv()

        @pl.when(event <= 4)
        def _():
            low_copy(event + 2, from_low.at[event]).start()

        high_copy(event, from_high.at[event]).wait_recv()

        @pl.when(event <= 4)
        def _():
            high_copy(event + 2, from_high.at[event]).start()

    arrive(0)

    def await_w(m):
        for item in w_copies(m):
            item.wait_recv()

    for m in range(2):
        if_sent(m, functools.partial(await_w, m))

    def core_copies(which):
        return (
            remote(
                w_kv.at[which], w_kv.at[which], core_send.at[0], core_recv.at[0], blk, other_core
            ),
            remote(w_q.at[which], w_q.at[which], core_send.at[1], core_recv.at[1], blk, other_core),
        )

    for item in core_copies(core):
        item.start()
    for item in core_copies(1 - core):
        item.wait_recv()

    lane = lax.broadcasted_iota(jnp.int32, (1, 128), 1)
    begin = jnp.zeros((1, 128), jnp.int32)
    end = jnp.zeros((1, 128), jnp.int32)
    start = jnp.int32(0)
    for c in range(8):
        stop = start + utt[c]
        begin = jnp.where(lane == 64 + c, start, begin)
        end = jnp.where(lane == 64 + c, stop, end)
        start = stop
    scale = math.log2(math.e) / 8.0

    def chunk_of(s, side):
        event = s + 7
        odd = event % 2
        away = jnp.where(s == 0, 0, jnp.where(s == 7, 4, (s + 1) // 2))
        if side == 0:
            return (z + 8 - away) % 8, jnp.where(s == 0, 0, odd)
        return (z + away) % 8, jnp.where(s == 0, 1, 1 - odd)

    def kv_copy(s):
        return remote(
            kv_stage.at[s], kv_land.at[s, pl.ds(rows, rows)], kv_send.at[s], kv_recv.at[s],
            partner, grp,
        )

    def q_copy(s):
        return remote(
            q_stage.at[s], q_land.at[s, pl.ds(rows, rows)], q_send.at[s], q_recv.at[s],
            partner, grp,
        )

    def times(values, weights):
        return lax.dot_general(
            values, weights, (((1,), (1,)), ((), ())), preferred_element_type=jnp.float32
        )

    def project(s):
        slot = (s + 7) % 8
        normed = jnp.concatenate([from_low[slot], from_high[slot]], axis=0)
        kv_stage[s] = times(normed, w_kv[1 - y_low]).astype(jnp.bfloat16)
        kv_copy(s).start()

        @pl.when(s < NEAR)
        def _():
            q_stage[s] = (times(normed, w_q[1 - y_low]) * scale).astype(jnp.bfloat16)
            q_copy(s).start()
            q_land[s, :rows] = (times(normed, w_q[y_low]) * scale).astype(jnp.bfloat16)

        kv_land[s, :rows] = times(normed, w_kv[y_low]).astype(jnp.bfloat16)

    def marks(s, piece):
        from_z, from_half = chunk_of(s, piece % 2)
        plane = y_low if piece < 2 else 1 - y_low
        first = grp * (16 * rows) + (from_z * 2 + plane) * rows + from_half * half
        position = lax.broadcasted_iota(jnp.int32, (half, 128), 0) + first
        return ((position >= begin) & (position < end)).astype(jnp.float32)

    def arrange(s):
        kv_copy(s).wait_recv()
        for piece in range(4):
            span = slice(piece * half, (piece + 1) * half)
            inside = marks(s, piece)
            for m in range(2):
                both = kv_land[s, span, m * 128 : (m + 1) * 128].astype(jnp.float32)
                keys[m, s, span] = jnp.where(lane < 64, both, inside).astype(jnp.bfloat16)
                vals[m, s, :, span] = jnp.where(lane < 64, 1.0, both).T.astype(jnp.bfloat16)

        @pl.when(s < NEAR)
        def _():
            q_copy(s).wait_recv()
            for piece in range(4):
                span = slice(piece * half, (piece + 1) * half)
                outside = jnp.where(lane < 72, (1.0 - marks(s, piece)) * big_negative, 0.0)
                both = q_land[s, span].astype(jnp.float32)
                query[0, s, span] = jnp.where(lane < 64, both, outside).astype(jnp.bfloat16)
                query[1, s, span] = jnp.where(lane < 64, pltpu.roll(both, 64, 1), outside).astype(
                    jnp.bfloat16
                )
            for m in range(2):
                peak[m, s] = jnp.full((1, 2 * rows), lowest, jnp.float32)
                mix[m, s] = jnp.zeros((128, 2 * rows), jnp.float32)

    def score(m, q, k):
        return times(keys[m, k], query[m, q])

    def absorb(m, q, k, buf):
        old = peak[m, q]
        new = jnp.maximum(old, jnp.max(buf[...], axis=0, keepdims=True))
        weights = jnp.exp2(buf[...] - new).astype(jnp.bfloat16)
        mix[m, q] = mix[m, q] * jnp.exp2(old - new) + jnp.dot(
            vals[m, k], weights, preferred_element_type=jnp.float32
        )
        peak[m, q] = new

    def pair(s, p):
        near = s < NEAR
        return (
            jnp.where(near, jnp.where(p <= s, s, p - s - 1), NEAR - 1 - p),
            jnp.where(near & (p <= s), p, s),
        )

    def both_heads(s, p):
        q, k = pair(s, p)
        buf_b[...] = score(1, q, k)
        absorb(0, q, k, buf_a)
        buf_a[...] = score(0, *pair(s, p + 1))
        absorb(1, q, k, buf_b)

    def last_heads(s, p):
        q, k = pair(s, p)
        buf_b[...] = score(1, q, k)
        absorb(0, q, k, buf_a)
        absorb(1, q, k, buf_b)

    def attend(s):
        count = jnp.where(s < NEAR, 2 * s + 1, NEAR)
        buf_a[...] = score(0, *pair(s, 0))

        def one(p, carry):
            both_heads(s, p)
            return carry

        lax.fori_loop(0, count - 1, one, 0)
        last_heads(s, count - 1)

    def step(s, carry):
        @pl.when((s >= 2) & (s < SETS))
        def _():
            arrive(s - 1)

        @pl.when(s < SETS)
        def _():
            project(s)

        @pl.when(s >= 2)
        def _():
            arrange(s - 2)
            attend(s - 2)

        return carry

    lax.fori_loop(0, SETS + 1, step, 0)

    slot_of_mine = quad * 2 + y_low

    def place_of(slot, at_half):
        return attended.at[
            pl.ds(pl.multiple_of(at_half * half, half), half),
            pl.ds(pl.multiple_of(slot * 128, 128), 128),
        ]

    def out_copy(s, piece):
        to_z, to_half = chunk_of(s, piece % 2)
        plane = y_low if piece < 2 else 1 - y_low
        return remote(
            out_stage.at[s, piece], place_of(slot_of_mine, to_half), out_send.at[s, piece],
            out_recv.at[s, piece], to_z * 2 + plane, grp,
        )

    def finish(s):
        packed = jnp.concatenate(
            [mix[m, s, 64:] / mix[m, s, :1] for m in range(2)], axis=0
        ).T.astype(jnp.bfloat16)

        @pl.when(s > 0)
        def _():
            for piece in range(2):
                out_stage[s, piece] = packed[piece * half : (piece + 1) * half]
                out_copy(s, piece).start()

        @pl.when(s == 0)
        def _():
            mine = pl.ds(pl.multiple_of(slot_of_mine * 128, 128), 128)
            attended[:rows, mine] = packed[:rows]

        for piece in range(2, 4):
            out_stage[s, piece] = packed[piece * half : (piece + 1) * half]
            out_copy(s, piece).start()

    last = SETS - 1
    arrange(last)
    buf_a[...] = score(0, *pair(last, 0))

    def release(p, carry):
        both_heads(last, p)
        finish(pair(last, p)[0])
        return carry

    lax.fori_loop(0, NEAR - 1, release, 0)
    last_heads(last, NEAR - 1)
    finish(0)
    for item in loads[1:2] + loads[5:]:
        item.wait()

    def collect(s, carry):
        for piece in range(4):
            plane = y_low if piece < 2 else 1 - y_low
            from_z, _ = chunk_of(s, 1 - piece % 2)
            _, at_half = chunk_of(s, piece % 2)
            got = remote(
                out_stage.at[s, piece], place_of(from_z % 4 * 2 + plane, at_half),
                out_send.at[s, piece], out_recv.at[s, piece], from_z * 2 + plane, grp,
            )

            def settle(got=got):
                got.wait_recv()
                got.wait_send()

            if piece < 2:
                pl.when(s > 0)(settle)
            else:
                settle()
        return carry

    lax.fori_loop(0, NEAR, collect, 0)

    added = (
        own[...].astype(jnp.float32) + jnp.dot(attended[...], w_out[...], preferred_element_type=jnp.float32)
    ).astype(jnp.bfloat16)
    residual[...] = added
    conv_in = normalize(added.astype(jnp.float32), conv_gain[...]).astype(jnp.bfloat16)
    width = added.shape[1]
    columns = width // 128
    for column in range(0, width, 256):
        values = jnp.dot(
            conv_in, w_glu[:, column : column + 256], preferred_element_type=jnp.float32
        )
        gates = jnp.dot(
            conv_in, w_glu[:, width + column : width + column + 256],
            preferred_element_type=jnp.float32,
        )
        gated = (values * jax.nn.sigmoid(gates)).astype(jnp.bfloat16)
        edge_out[0, :, column : column + 256] = gated[:HALO]
        edge_out[1, :, column : column + 256] = gated[rows - HALO :]
        wide = gated.astype(jnp.float32)
        for c in range(2):
            tall[column // 128 + c, HALO : HALO + rows] = wide[:, c * 128 : (c + 1) * 128]

    to_left = remote(edge_out.at[0], edge_in.at[1], halo_send.at[0], halo_recv.at[0], *left)
    to_right = remote(edge_out.at[1], edge_in.at[0], halo_send.at[1], halo_recv.at[1], *right)
    to_left.start()
    to_right.start()

    taps = w_depth.shape[0]
    reach = taps // 2
    block = 64
    first_frame = (grp * 16 + blk) * rows

    def convolve(base):
        at = lax.broadcasted_iota(jnp.int32, (block, 128), 0) + (first_frame + base)
        first = jnp.zeros((block, 128), jnp.int32)
        final = jnp.zeros((block, 128), jnp.int32)
        begun = jnp.int32(0)
        for c in range(8):
            over = begun + utt[c]
            first = jnp.where(at >= begun, begun, first)
            final = jnp.where(at >= begun, over, final)
            begun = over
        first_tap = first - at + reach
        last_tap = final - at + reach
        for t in range(taps):
            valid[t] = jnp.where((first_tap <= t) & (last_tap > t), 1.0, 0.0)

        def column_of(c, carry):
            total = jnp.zeros((block, 128), jnp.float32)
            for t in range(taps):
                total = total + (
                    tall[c, pl.ds(base + (HALO - reach + t), block)] * valid[t]
                    * w_depth[t : t + 1, pl.ds(pl.multiple_of(c * 128, 128), 128)]
                )
            mixed[c] = total
            return carry

        lax.fori_loop(0, columns, column_of, 0)
        pieces = [mixed[c] for c in range(columns)]
        mean = jnp.sum(functools.reduce(jnp.add, pieces), axis=1, keepdims=True) / width
        pieces = [piece - mean for piece in pieces]
        spread = (
            jnp.sum(functools.reduce(jnp.add, [p * p for p in pieces]), axis=1, keepdims=True)
            / width
        )
        factor = lax.rsqrt(spread + epsilon)
        for c in range(columns):
            span = slice(c * 128, (c + 1) * 128)
            value = pieces[c] * factor * depth_gain[:, span]
            activated[pl.ds(base, block), span] = (value * jax.nn.sigmoid(value)).astype(
                jnp.bfloat16
            )

    def conv_step(index, carry):
        @pl.when(index == rows // block - 2)
        def _():
            to_left.wait_recv()
            to_right.wait_recv()
            for c in range(columns):
                span = slice(c * 128, (c + 1) * 128)
                tall[c, :HALO] = edge_in[0, :, span].astype(jnp.float32)
                tall[c, HALO + rows :] = edge_in[1, :, span].astype(jnp.float32)

        convolve(pl.multiple_of((index + 1) % (rows // block) * block, block))
        return carry

    lax.fori_loop(0, rows // block, conv_step, 0)
    for column in range(0, width, 256):
        span = slice(column, column + 256)
        out_ref[:, span] = (
            residual[:, span].astype(jnp.float32)
            + jnp.dot(activated[...], w_proj[:, span], preferred_element_type=jnp.float32)
        ).astype(jnp.bfloat16)

    for event in range(7):
        low_copy(event, from_low.at[event]).wait_send()
        high_copy(event, from_high.at[event]).wait_send()
    for s in range(SETS):
        kv_copy(s).wait_send()
    for s in range(NEAR):
        q_copy(s).wait_send()
    for item in core_copies(core):
        item.wait_send()

    def sent_w(m):
        for item in w_copies(m):
            item.wait_send()

    for m in range(2):
        if_direct(m, functools.partial(sent_w, m))

    @pl.when(even)
    def _():
        for item in (*relay_copies(), *far_copies()):
            item.wait_send()

    to_left.wait_send()
    to_right.wait_send()


def block_of(
    frames, utt_lengths, attn_gain, w_qkv, w_out, conv_gain, w_glu, w_depth, depth_gain, w_proj
):
    rows, width = frames.shape
    half = rows // 2
    columns = width // 128
    taps = w_depth.shape[0]
    hbm = pl.BlockSpec(memory_space=pltpu.HBM)
    dma = pltpu.SemaphoreType.DMA
    bf16, f32 = jnp.bfloat16, jnp.float32
    return pl.pallas_call(
        mixing_kernel,
        out_shape=jax.ShapeDtypeStruct((rows, width), bf16),
        in_specs=[hbm] * 10,
        out_specs=pl.BlockSpec(memory_space=pltpu.VMEM),
        scratch_shapes=[
            pltpu.SMEM((8,), jnp.int32),
            pltpu.VMEM((1, width), f32),
            pltpu.VMEM((1, width), f32),
            pltpu.VMEM((1, width), f32),
            pltpu.VMEM((192, width), bf16),
            pltpu.VMEM((width, width), bf16),
            pltpu.VMEM((width, 2 * width), bf16),
            pltpu.VMEM((taps, width), f32),
            pltpu.VMEM((width, width), bf16),
            pltpu.VMEM((rows, width), bf16),
            pltpu.VMEM((8, half, width), bf16),
            pltpu.VMEM((8, half, width), bf16),
            pltpu.VMEM((192, width), bf16),
            pltpu.VMEM((2, 256, width), bf16),
            pltpu.VMEM((2, 128, width), bf16),
            pltpu.VMEM((SETS, rows, 256), bf16),
            pltpu.VMEM((NEAR, rows, 128), bf16),
            pltpu.VMEM((SETS, 2 * rows, 256), bf16),
            pltpu.VMEM((NEAR, 2 * rows, 128), bf16),
            pltpu.VMEM((2, NEAR, 2 * rows, 128), bf16),
            pltpu.VMEM((2, SETS, 2 * rows, 128), bf16),
            pltpu.VMEM((2, SETS, 128, 2 * rows), bf16),
            pltpu.VMEM((2, NEAR, 1, 2 * rows), f32),
            pltpu.VMEM((2, NEAR, 128, 2 * rows), f32),
            pltpu.VMEM((2 * rows, 2 * rows), f32),
            pltpu.VMEM((2 * rows, 2 * rows), f32),
            pltpu.VMEM((NEAR, 4, half, 128), bf16),
            pltpu.VMEM((rows, width), bf16),
            pltpu.VMEM((rows, width), bf16),
            pltpu.VMEM((rows, width), bf16),
            pltpu.VMEM((2, HALO, width), bf16),
            pltpu.VMEM((2, HALO, width), bf16),
            pltpu.VMEM((columns, rows + 2 * HALO, 128), f32),
            pltpu.VMEM((taps, 64, 128), f32),
            pltpu.VMEM((columns, 64, 128), f32),
            dma((26,)),
            dma((7,)), dma((7,)), dma((7,)), dma((7,)),
            dma((2, 2)), dma((2, 2)), dma((2,)), dma((2,)), dma((2,)), dma((2,)), dma((2,)),
            dma((SETS,)), dma((SETS,)), dma((NEAR,)), dma((NEAR,)),
            dma((NEAR, 4)), dma((NEAR, 4)),
            dma((2,)), dma((2,)),
        ],
        compiler_params=pltpu.CompilerParams(
            collective_id=0, has_side_effects=True, vmem_limit_bytes=67043328
        ),
    )(
        utt_lengths, frames, attn_gain.reshape(1, width), w_qkv.T, w_out,
        conv_gain.reshape(1, width), w_glu, w_depth, depth_gain.reshape(1, width), w_proj,
    )


def body(frames, *others):
    return block_of(frames[0], *others)[None]


def solution(mesh):
    in_specs = (P("grp", "blk", None), P(), P(), P(None, "grp"), P(), P(), P(), P(), P(), P())
    out_specs = P("grp", "blk", None)
    return jax.shard_map(body, mesh=mesh, in_specs=in_specs, out_specs=out_specs, check_vma=False)
```

```python
import functools
import math

import jax
import jax.numpy as jnp
from jax import lax
from jax.experimental import pallas as pl
from jax.experimental.pallas import tpu as pltpu
from jax.sharding import PartitionSpec as P

SETS = 8
NEAR = 4
HALO = 16
MESH = pl.DeviceIdType.MESH

epsilon = 1e-05
big_negative = -1e30
lowest = -2e38


def normalize(values, row_gain):
    center = values - jnp.mean(values, axis=-1, keepdims=True)
    spread = jnp.mean(center * center, axis=-1, keepdims=True)
    return center * lax.rsqrt(spread + epsilon) * row_gain


def mixing_kernel(
    utt_hbm, frames_hbm, gain_hbm, w_hbm, w_out_hbm, conv_gain_hbm, w_glu_hbm, w_depth_hbm,
    depth_gain_hbm, w_proj_hbm,
    out_ref,
    utt, gain, conv_gain, depth_gain, w_mine, w_out, w_glu, w_depth, w_proj,
    own, from_low, from_high, w_relay, w_kv, w_q, kv_stage, q_stage, kv_land, q_land, query, keys, vals,
    peak, mix, buf_a, buf_b, out_stage, attended, activated, residual, edge_out, edge_in, tall, valid, mixed,
    load_sem, low_send, low_recv, high_send, high_recv, w_send, w_recv, relay_send, relay_recv,
    far_send, core_send, core_recv,
    kv_send, kv_recv, q_send, q_recv, out_send, out_recv, halo_send, halo_recv,
):
    half = from_low.shape[1]
    rows = 2 * half
    blk = lax.axis_index("blk")
    grp = lax.axis_index("grp")
    z, y_low = blk // 2, blk % 2
    x, y_high, core = grp // 4, (grp // 2) % 2, grp % 2
    quad = z % 4

    def member(of_quad, m):
        return (of_quad + 2 * m) % 4, m

    def head_of(of_quad, m, of_core):
        right_by, across = member(of_quad, m)
        return ((x + right_by) % 4) * 4 + ((y_high + across) % 2) * 2 + of_core

    other_core = grp + 1 - 2 * core
    partner = blk + 1 - 2 * y_low

    def w_from(m):
        return jnp.where(member(quad, m)[1] == 1, partner, blk), head_of(quad, m, core)

    def w_to(m):
        right_by, across = member(quad, m)
        return (
            jnp.where(across == 1, partner, blk),
            ((x + 4 - right_by) % 4) * 4 + ((y_high + across) % 2) * 2 + core,
        )

    even = quad % 2 == 0
    far = jnp.where(quad == 0, 1, 0)
    stride = jnp.where(core == 0, 3, 1)

    def along(count, across):
        return (
            jnp.where(across == 1, partner, blk),
            ((x + count) % 4) * 4 + ((y_high + across) % 2) * 2 + core,
        )

    relay_to, relay_from = along(stride, 0), along(4 - stride, 0)
    far_to, far_from = along(stride, far), along(4 - stride, far)

    def if_direct(m, act):
        pl.when(quad > 0 if m == 1 else quad % 2 == 1)(act)

    def if_sent(m, act):
        if m == 1:
            act()
        else:
            pl.when(quad > 0)(act)

    z_up = (blk + 2) % 16
    z_down = (blk + 14) % 16
    left = ((blk + 15) % 16, (grp + jnp.where(blk == 0, 15, 0)) % 16)
    right = ((blk + 1) % 16, (grp + jnp.where(blk == 15, 1, 0)) % 16)

    def place(b, g):
        return {"blk": b, "grp": g}

    def load(index, src, dst):
        return pltpu.make_async_copy(src, dst, load_sem.at[index])

    loads = [
        load(0, frames_hbm, own),
        load(1, conv_gain_hbm, conv_gain),
        load(2, w_hbm, w_mine),
        load(3, gain_hbm, gain),
        load(4, utt_hbm, utt),
        load(7, w_glu_hbm, w_glu),
        load(8, w_depth_hbm, w_depth),
        load(9, depth_gain_hbm, depth_gain),
        load(6, w_proj_hbm, w_proj),
    ]
    for slot in range(SETS):
        for m in range(2):
            head = head_of(slot // 2, m, slot % 2)
            loads.append(
                load(
                    10 + 2 * slot + m,
                    w_out_hbm.at[pl.ds(pl.multiple_of(head * 64, 64), 64)],
                    w_out.at[pl.ds(slot * 128 + m * 64, 64)],
                )
            )
    for item in loads:
        item.start()

    barrier = pltpu.get_barrier_semaphore()

    def greet(b, g):
        pl.semaphore_signal(barrier, inc=1, device_id=place(b, g), device_id_type=MESH)

    for step in range(1, 16):
        greet((blk + step) % 16, grp)
    greet(blk, other_core)
    greet(*left)
    greet(*right)

    for m in range(2):
        def greet_both(m=m):
            greet(*w_to(m))
            greet(*w_from(m))

        if_direct(m, greet_both)

    @pl.when(even)
    def _():
        for each in (relay_to, relay_from, far_to, far_from):
            greet(*each)

    loads[0].wait()
    loads[3].wait()
    for side, kept in ((0, from_low), (1, from_high)):
        kept[7] = normalize(
            own[side * half : (side + 1) * half].astype(jnp.float32), gain[...]
        ).astype(jnp.bfloat16)
    loads[2].wait()
    pl.semaphore_wait(barrier, jnp.where(quad == 2, 24, 22))

    def remote(src, dst, send, recv, b, g):
        return pltpu.make_async_remote_copy(
            src_ref=src, dst_ref=dst, send_sem=send, recv_sem=recv,
            device_id=place(b, g), device_id_type=MESH,
        )

    def low_copy(event, src):
        return remote(src, from_low.at[event], low_send.at[event], low_recv.at[event], z_up, grp)

    def high_copy(event, src):
        return remote(
            src, from_high.at[event], high_send.at[event], high_recv.at[event], z_down, grp
        )

    low_copy(0, from_low.at[7]).start()
    high_copy(0, from_high.at[7]).start()
    low_copy(1, from_high.at[7]).start()
    high_copy(1, from_low.at[7]).start()

    def w_copies(m):
        return (
            remote(
                w_mine.at[pl.ds(64, 128)], w_kv.at[core, pl.ds(m * 128, 128)],
                w_send.at[m, 0], w_recv.at[m, 0], *w_to(m),
            ),
            remote(
                w_mine.at[pl.ds(0, 64)], w_q.at[core, pl.ds(m * 64, 64)],
                w_send.at[m, 1], w_recv.at[m, 1], *w_to(m),
            ),
        )

    def start_w(m):
        for item in w_copies(m):
            item.start()

    def relay_copies():
        return [
            remote(
                w_mine.at[at], w_relay.at[at], relay_send.at[part], relay_recv.at[part], *relay_to
            )
            for part, at in enumerate((pl.ds(64, 128), pl.ds(0, 64)))
        ]

    def far_copies():
        return (
            remote(
                w_relay.at[pl.ds(64, 128)],
                w_kv.at[core, pl.ds(pl.multiple_of(far * 128, 128), 128)],
                far_send.at[0], w_recv.at[far, 0], *far_to,
            ),
            remote(
                w_relay.at[pl.ds(0, 64)],
                w_q.at[core, pl.ds(pl.multiple_of(far * 64, 64), 64)],
                far_send.at[1], w_recv.at[far, 1], *far_to,
            ),
        )

    @pl.when(even)
    def _():
        for item in relay_copies():
            item.start()

    for m in range(2):
        if_direct(m, functools.partial(start_w, m))

    @pl.when(quad == 0)
    def _():
        w_kv[core, :128] = w_mine[64:]
        w_q[core, :64] = w_mine[:64]

    @pl.when(even)
    def _():
        for came, item in zip(relay_copies(), far_copies()):
            came.wait_recv()
            item.start()

    loads[4].wait()

    def arrive(event):
        low_copy(event, from_low.at[event]).wait_recv()

        @pl.when(event <= 4)
        def _():
            low_copy(event + 2, from_low.at[event]).start()

        high_copy(event, from_high.at[event]).wait_recv()

        @pl.when(event <= 4)
        def _():
            high_copy(event + 2, from_high.at[event]).start()

    arrive(0)

    def await_w(m):
        for item in w_copies(m):
            item.wait_recv()

    for m in range(2):
        if_sent(m, functools.partial(await_w, m))

    def core_copies(which):
        return (
            remote(
                w_kv.at[which], w_kv.at[which], core_send.at[0], core_recv.at[0], blk, other_core
            ),
            remote(w_q.at[which], w_q.at[which], core_send.at[1], core_recv.at[1], blk, other_core),
        )

    for item in core_copies(core):
        item.start()
    for item in core_copies(1 - core):
        item.wait_recv()

    lane = lax.broadcasted_iota(jnp.int32, (1, 128), 1)
    begin = jnp.zeros((1, 128), jnp.int32)
    end = jnp.zeros((1, 128), jnp.int32)
    start = jnp.int32(0)
    for c in range(8):
        stop = start + utt[c]
        begin = jnp.where(lane == 64 + c, start, begin)
        end = jnp.where(lane == 64 + c, stop, end)
        start = stop
    scale = math.log2(math.e) / 8.0

    def chunk_of(s, side):
        event = s + 7
        odd = event % 2
        away = jnp.where(s == 0, 0, jnp.where(s == 7, 4, (s + 1) // 2))
        if side == 0:
            return (z + 8 - away) % 8, jnp.where(s == 0, 0, odd)
        return (z + away) % 8, jnp.where(s == 0, 1, 1 - odd)

    def kv_copy(s):
        return remote(
            kv_stage.at[s], kv_land.at[s, pl.ds(rows, rows)], kv_send.at[s], kv_recv.at[s],
            partner, grp,
        )

    def q_copy(s):
        return remote(
            q_stage.at[s], q_land.at[s, pl.ds(rows, rows)], q_send.at[s], q_recv.at[s],
            partner, grp,
        )

    def times(values, weights):
        return lax.dot_general(
            values, weights, (((1,), (1,)), ((), ())), preferred_element_type=jnp.float32
        )

    def project(s):
        slot = (s + 7) % 8
        normed = jnp.concatenate([from_low[slot], from_high[slot]], axis=0)
        kv_stage[s] = times(normed, w_kv[1 - y_low]).astype(jnp.bfloat16)
        kv_copy(s).start()

        @pl.when(s < NEAR)
        def _():
            q_stage[s] = (times(normed, w_q[1 - y_low]) * scale).astype(jnp.bfloat16)
            q_copy(s).start()
            q_land[s, :rows] = (times(normed, w_q[y_low]) * scale).astype(jnp.bfloat16)

        kv_land[s, :rows] = times(normed, w_kv[y_low]).astype(jnp.bfloat16)

    def marks(s, piece):
        from_z, from_half = chunk_of(s, piece % 2)
        plane = y_low if piece < 2 else 1 - y_low
        first = grp * (16 * rows) + (from_z * 2 + plane) * rows + from_half * half
        position = lax.broadcasted_iota(jnp.int32, (half, 128), 0) + first
        return ((position >= begin) & (position < end)).astype(jnp.float32)

    def arrange(s):
        kv_copy(s).wait_recv()
        for piece in range(4):
            span = slice(piece * half, (piece + 1) * half)
            inside = marks(s, piece)
            for m in range(2):
                both = kv_land[s, span, m * 128 : (m + 1) * 128].astype(jnp.float32)
                keys[m, s, span] = jnp.where(lane < 64, both, inside).astype(jnp.bfloat16)
                vals[m, s, :, span] = jnp.where(lane < 64, 1.0, both).T.astype(jnp.bfloat16)

        @pl.when(s < NEAR)
        def _():
            q_copy(s).wait_recv()
            for piece in range(4):
                span = slice(piece * half, (piece + 1) * half)
                outside = jnp.where(lane < 72, (1.0 - marks(s, piece)) * big_negative, 0.0)
                both = q_land[s, span].astype(jnp.float32)
                query[0, s, span] = jnp.where(lane < 64, both, outside).astype(jnp.bfloat16)
                query[1, s, span] = jnp.where(lane < 64, pltpu.roll(both, 64, 1), outside).astype(
                    jnp.bfloat16
                )
            for m in range(2):
                peak[m, s] = jnp.full((1, 2 * rows), lowest, jnp.float32)
                mix[m, s] = jnp.zeros((128, 2 * rows), jnp.float32)

    def score(m, q, k):
        return times(keys[m, k], query[m, q])

    def absorb(m, q, k, buf):
        old = peak[m, q]
        new = jnp.maximum(old, jnp.max(buf[...], axis=0, keepdims=True))
        weights = jnp.exp2(buf[...] - new).astype(jnp.bfloat16)
        mix[m, q] = mix[m, q] * jnp.exp2(old - new) + jnp.dot(
            vals[m, k], weights, preferred_element_type=jnp.float32
        )
        peak[m, q] = new

    def pair(s, p):
        near = s < NEAR
        return (
            jnp.where(near, jnp.where(p <= s, s, p - s - 1), NEAR - 1 - p),
            jnp.where(near & (p <= s), p, s),
        )

    def both_heads(s, p):
        q, k = pair(s, p)
        buf_b[...] = score(1, q, k)
        absorb(0, q, k, buf_a)
        buf_a[...] = score(0, *pair(s, p + 1))
        absorb(1, q, k, buf_b)

    def last_heads(s, p):
        q, k = pair(s, p)
        buf_b[...] = score(1, q, k)
        absorb(0, q, k, buf_a)
        absorb(1, q, k, buf_b)

    def attend(s):
        count = jnp.where(s < NEAR, 2 * s + 1, NEAR)
        buf_a[...] = score(0, *pair(s, 0))

        def one(p, carry):
            both_heads(s, p)
            return carry

        lax.fori_loop(0, count - 1, one, 0)
        last_heads(s, count - 1)

    def step(s, carry):
        @pl.when((s >= 2) & (s < SETS))
        def _():
            arrive(s - 1)

        @pl.when(s < SETS)
        def _():
            project(s)

        @pl.when(s >= 2)
        def _():
            arrange(s - 2)
            attend(s - 2)

        return carry

    lax.fori_loop(0, SETS + 1, step, 0)

    slot_of_mine = quad * 2 + y_low

    def place_of(slot, at_half):
        return attended.at[
            pl.ds(pl.multiple_of(at_half * half, half), half),
            pl.ds(pl.multiple_of(slot * 128, 128), 128),
        ]

    def out_copy(s, piece):
        to_z, to_half = chunk_of(s, piece % 2)
        plane = y_low if piece < 2 else 1 - y_low
        return remote(
            out_stage.at[s, piece], place_of(slot_of_mine, to_half), out_send.at[s, piece],
            out_recv.at[s, piece], to_z * 2 + plane, grp,
        )

    def finish(s):
        packed = jnp.concatenate(
            [mix[m, s, 64:] / mix[m, s, :1] for m in range(2)], axis=0
        ).T.astype(jnp.bfloat16)

        @pl.when(s > 0)
        def _():
            for piece in range(2):
                out_stage[s, piece] = packed[piece * half : (piece + 1) * half]
                out_copy(s, piece).start()

        @pl.when(s == 0)
        def _():
            mine = pl.ds(pl.multiple_of(slot_of_mine * 128, 128), 128)
            attended[:rows, mine] = packed[:rows]

        for piece in range(2, 4):
            out_stage[s, piece] = packed[piece * half : (piece + 1) * half]
            out_copy(s, piece).start()

    last = SETS - 1
    arrange(last)
    buf_a[...] = score(0, *pair(last, 0))

    def release(p, carry):
        both_heads(last, p)
        finish(pair(last, p)[0])
        return carry

    lax.fori_loop(0, NEAR - 1, release, 0)
    last_heads(last, NEAR - 1)
    finish(0)
    for item in loads[1:2] + loads[5:]:
        item.wait()

    taps = w_depth.shape[0]
    reach = taps // 2
    block = 64
    first_frame = (grp * 16 + blk) * rows

    def mark_taps(part, carry):
        at = lax.broadcasted_iota(jnp.int32, (block, 128), 0) + (first_frame + part * block)
        first = jnp.zeros((block, 128), jnp.int32)
        final = jnp.zeros((block, 128), jnp.int32)
        begun = jnp.int32(0)
        for c in range(8):
            over = begun + utt[c]
            first = jnp.where(at >= begun, begun, first)
            final = jnp.where(at >= begun, over, final)
            begun = over
        first_tap = first - at + reach
        last_tap = final - at + reach
        for t in range(taps):
            valid[part, t] = jnp.where((first_tap <= t) & (last_tap > t), 1.0, 0.0)
        return carry

    lax.fori_loop(0, rows // block, mark_taps, 0)

    def collect(s, carry):
        for piece in range(4):
            plane = y_low if piece < 2 else 1 - y_low
            from_z, _ = chunk_of(s, 1 - piece % 2)
            _, at_half = chunk_of(s, piece % 2)
            got = remote(
                out_stage.at[s, piece], place_of(from_z % 4 * 2 + plane, at_half),
                out_send.at[s, piece], out_recv.at[s, piece], from_z * 2 + plane, grp,
            )

            def settle(got=got):
                got.wait_recv()
                got.wait_send()

            if piece < 2:
                pl.when(s > 0)(settle)
            else:
                settle()
        return carry

    lax.fori_loop(0, NEAR, collect, 0)

    added = (
        own[...].astype(jnp.float32) + jnp.dot(attended[...], w_out[...], preferred_element_type=jnp.float32)
    ).astype(jnp.bfloat16)
    residual[...] = added
    conv_in = normalize(added.astype(jnp.float32), conv_gain[...]).astype(jnp.bfloat16)
    width = added.shape[1]
    columns = width // 128
    for column in range(0, width, 256):
        values = jnp.dot(
            conv_in, w_glu[:, column : column + 256], preferred_element_type=jnp.float32
        )
        gates = jnp.dot(
            conv_in, w_glu[:, width + column : width + column + 256],
            preferred_element_type=jnp.float32,
        )
        gated = (values * jax.nn.sigmoid(gates)).astype(jnp.bfloat16)
        edge_out[0, :, column : column + 256] = gated[:HALO]
        edge_out[1, :, column : column + 256] = gated[rows - HALO :]
        wide = gated.astype(jnp.float32)
        for c in range(2):
            tall[column // 128 + c, HALO : HALO + rows] = wide[:, c * 128 : (c + 1) * 128]

    to_left = remote(edge_out.at[0], edge_in.at[1], halo_send.at[0], halo_recv.at[0], *left)
    to_right = remote(edge_out.at[1], edge_in.at[0], halo_send.at[1], halo_recv.at[1], *right)
    to_left.start()
    to_right.start()

    def convolve(base):
        def column_of(c, carry):
            total = jnp.zeros((block, 128), jnp.float32)
            for t in range(taps):
                total = total + (
                    tall[c, pl.ds(base + (HALO - reach + t), block)] * valid[base // block, t]
                    * w_depth[t : t + 1, pl.ds(pl.multiple_of(c * 128, 128), 128)]
                )
            mixed[c] = total
            return carry

        lax.fori_loop(0, columns, column_of, 0)
        pieces = [mixed[c] for c in range(columns)]
        mean = jnp.sum(functools.reduce(jnp.add, pieces), axis=1, keepdims=True) / width
        pieces = [piece - mean for piece in pieces]
        spread = (
            jnp.sum(functools.reduce(jnp.add, [p * p for p in pieces]), axis=1, keepdims=True)
            / width
        )
        factor = lax.rsqrt(spread + epsilon)
        for c in range(columns):
            span = slice(c * 128, (c + 1) * 128)
            value = pieces[c] * factor * depth_gain[:, span]
            activated[pl.ds(base, block), span] = (value * jax.nn.sigmoid(value)).astype(
                jnp.bfloat16
            )

    def conv_step(index, carry):
        @pl.when(index == rows // block - 2)
        def _():
            to_left.wait_recv()
            to_right.wait_recv()
            for c in range(columns):
                span = slice(c * 128, (c + 1) * 128)
                tall[c, :HALO] = edge_in[0, :, span].astype(jnp.float32)
                tall[c, HALO + rows :] = edge_in[1, :, span].astype(jnp.float32)

        convolve(pl.multiple_of((index + 1) % (rows // block) * block, block))
        return carry

    lax.fori_loop(0, rows // block, conv_step, 0)
    for column in range(0, width, 256):
        span = slice(column, column + 256)
        out_ref[:, span] = (
            residual[:, span].astype(jnp.float32)
            + jnp.dot(activated[...], w_proj[:, span], preferred_element_type=jnp.float32)
        ).astype(jnp.bfloat16)

    for event in range(7):
        low_copy(event, from_low.at[event]).wait_send()
        high_copy(event, from_high.at[event]).wait_send()
    for s in range(SETS):
        kv_copy(s).wait_send()
    for s in range(NEAR):
        q_copy(s).wait_send()
    for item in core_copies(core):
        item.wait_send()

    def sent_w(m):
        for item in w_copies(m):
            item.wait_send()

    for m in range(2):
        if_direct(m, functools.partial(sent_w, m))

    @pl.when(even)
    def _():
        for item in (*relay_copies(), *far_copies()):
            item.wait_send()

    to_left.wait_send()
    to_right.wait_send()


def block_of(
    frames, utt_lengths, attn_gain, w_qkv, w_out, conv_gain, w_glu, w_depth, depth_gain, w_proj
):
    rows, width = frames.shape
    half = rows // 2
    columns = width // 128
    taps = w_depth.shape[0]
    hbm = pl.BlockSpec(memory_space=pltpu.HBM)
    dma = pltpu.SemaphoreType.DMA
    bf16, f32 = jnp.bfloat16, jnp.float32
    return pl.pallas_call(
        mixing_kernel,
        out_shape=jax.ShapeDtypeStruct((rows, width), bf16),
        in_specs=[hbm] * 10,
        out_specs=pl.BlockSpec(memory_space=pltpu.VMEM),
        scratch_shapes=[
            pltpu.SMEM((8,), jnp.int32),
            pltpu.VMEM((1, width), f32),
            pltpu.VMEM((1, width), f32),
            pltpu.VMEM((1, width), f32),
            pltpu.VMEM((192, width), bf16),
            pltpu.VMEM((width, width), bf16),
            pltpu.VMEM((width, 2 * width), bf16),
            pltpu.VMEM((taps, width), f32),
            pltpu.VMEM((width, width), bf16),
            pltpu.VMEM((rows, width), bf16),
            pltpu.VMEM((8, half, width), bf16),
            pltpu.VMEM((8, half, width), bf16),
            pltpu.VMEM((192, width), bf16),
            pltpu.VMEM((2, 256, width), bf16),
            pltpu.VMEM((2, 128, width), bf16),
            pltpu.VMEM((SETS, rows, 256), bf16),
            pltpu.VMEM((NEAR, rows, 128), bf16),
            pltpu.VMEM((SETS, 2 * rows, 256), bf16),
            pltpu.VMEM((NEAR, 2 * rows, 128), bf16),
            pltpu.VMEM((2, NEAR, 2 * rows, 128), bf16),
            pltpu.VMEM((2, SETS, 2 * rows, 128), bf16),
            pltpu.VMEM((2, SETS, 128, 2 * rows), bf16),
            pltpu.VMEM((2, NEAR, 1, 2 * rows), f32),
            pltpu.VMEM((2, NEAR, 128, 2 * rows), f32),
            pltpu.VMEM((2 * rows, 2 * rows), f32),
            pltpu.VMEM((2 * rows, 2 * rows), f32),
            pltpu.VMEM((NEAR, 4, half, 128), bf16),
            pltpu.VMEM((rows, width), bf16),
            pltpu.VMEM((rows, width), bf16),
            pltpu.VMEM((rows, width), bf16),
            pltpu.VMEM((2, HALO, width), bf16),
            pltpu.VMEM((2, HALO, width), bf16),
            pltpu.VMEM((columns, rows + 2 * HALO, 128), f32),
            pltpu.VMEM((rows // 64, taps, 64, 128), f32),
            pltpu.VMEM((columns, 64, 128), f32),
            dma((26,)),
            dma((7,)), dma((7,)), dma((7,)), dma((7,)),
            dma((2, 2)), dma((2, 2)), dma((2,)), dma((2,)), dma((2,)), dma((2,)), dma((2,)),
            dma((SETS,)), dma((SETS,)), dma((NEAR,)), dma((NEAR,)),
            dma((NEAR, 4)), dma((NEAR, 4)),
            dma((2,)), dma((2,)),
        ],
        compiler_params=pltpu.CompilerParams(
            collective_id=0, has_side_effects=True, vmem_limit_bytes=67043328
        ),
    )(
        utt_lengths, frames, attn_gain.reshape(1, width), w_qkv.T, w_out,
        conv_gain.reshape(1, width), w_glu, w_depth, depth_gain.reshape(1, width), w_proj,
    )


def body(frames, *others):
    return block_of(frames[0], *others)[None]


def solution(mesh):
    in_specs = (P("grp", "blk", None), P(), P(), P(None, "grp"), P(), P(), P(), P(), P(), P())
    out_specs = P("grp", "blk", None)
    return jax.shard_map(body, mesh=mesh, in_specs=in_specs, out_specs=out_specs, check_vma=False)
```
